32 devices in a mesh: row: 4 (over x, core), col: 4 (over z), depth: 2 (over y).
Axes of the slice: x: 2, y: 2, z: 4, core: 2. Of those that a mesh axis runs over, the one named last changes fastest.
Arguments:
- acts: bfloat16 [256, 32768], P('depth', 'row'), may hold values from -6 to 6
- act_mask: int32 [256, 256], P('depth', 'row'), may hold values 0 or 1
- w1: bfloat16 [256, 32, 128, 128], P(('row', 'depth'), 'col'), may hold values from -0.09375 to 0.09375
- cols1: int32 [256, 32], P('row', 'col'), may hold values from 0 to 255, as said below
- bias1: float32 [32768], P('col'), may hold values from -3 to 3
- mask2: int32 [256, 256], P('depth', 'col'), may hold values 0 or 1
- w2: bfloat16 [256, 32, 128, 128], P(('col', 'depth'), 'row'), may hold values from -0.1875 to 0.1875
- cols2: int32 [256, 32], P('col', 'row'), may hold values from 0 to 255, as said below
- bias2: float32 [32768], P(('row', 'col')), may hold values from -3 to 3
Outputs:
- result: bfloat16 [256, 32768], P('depth', ('row', 'col'))
The draws below stay inside these ranges and needn't reach their ends.
Inputs may be any that keep to these rules, and one draw needn't show every extreme that they name: `cols1`: in each of the 256 block rows the 32 entries name different block columns, and for every g the entries g * 8 to g * 8 + 7 lie among block columns g * 64 to g * 64 + 63. `cols2`: in each of the 256 block rows the 32 entries name different block columns, and for every g the entries g * 8 to g * 8 + 7 lie among block columns g * 64 to g * 64 + 63.
All inputs are finite; a program needn't handle non-finite values. No bound on the sum of `act_mask` or of `mask2` on one device may be relied on, other than what follows from the above.
Results may differ from the reference program's by a relative error of at most 0.0047.
Values may be sent and summed in bfloat16 or wider, within the bound.
A program may use at most 128 MiB of HBM per device.

```python
import jax
import jax.numpy as jnp
from jax import lax

N = 32768
BS = 128
K = 32
NB = 256
NB_COL = 64
NB_ROW = 64
KC = 8
KR = 8
M = 256


def pattern(key, extent, per_group):
    groups = NB // extent
    score_values = jax.random.randint(key, (NB, groups, extent), 0, 1 << 20, dtype=jnp.int32)
    score_values = score_values * extent + jnp.arange(extent, dtype=jnp.int32)
    ranked = jnp.argsort(score_values, axis=-1)[:, :, :per_group].astype(jnp.int32)
    placed = ranked + (jnp.arange(groups, dtype=jnp.int32) * extent)[None, :, None]
    return placed.reshape(NB, groups * per_group).astype(jnp.int32)


def draw_cols1(key, part):
    return pattern(jax.random.fold_in(key, 1), NB_COL, KC)


def draw_cols2(key, part):
    return pattern(jax.random.fold_in(key, 2), NB_ROW, KR)


def with_ends(entries, own_key, smallest, high):
    index_at = [jax.random.randint(jax.random.fold_in(own_key, axis), (), 0, length) for axis, length in enumerate(entries.shape)]
    longest = entries.shape.index(max(entries.shape))
    neighbour = index_at[:longest] + [(index_at[longest] + 1) % entries.shape[longest]] + index_at[longest + 1:]
    return entries.at[tuple(index_at)].set(smallest).at[tuple(neighbour)].set(high)


def level_of(stream_key, shape, cuts, low, high):
    level = 1.0
    for position, blocks in cuts:
        draws = jax.random.uniform(jax.random.fold_in(jax.random.fold_in(stream_key, 6), position), (blocks,), jnp.float32, low / len(cuts), high / len(cuts))
        level = level * jnp.repeat(jnp.exp(draws), shape[position] // blocks).reshape((-1,) + (1,) * (len(shape) - 1 - position))
    return level


def normal_values(rng, shape, scale, most, pieces=(), kind=jnp.bfloat16):
    drawn = jax.random.normal(rng, shape, jnp.float32) * scale
    if len(pieces) > 0:
        drawn = level_of(rng, shape, pieces, -0.22, 0.18) * drawn
    return jnp.clip(drawn, min=-most, max=most).astype(kind)


def setup_inputs(seed: int = 0) -> dict:
    arg_keys = jax.random.split(jax.random.key(seed), 10)
    return {
        "acts": normal_values(arg_keys[0], (M, N), 1.0, 6.0, ((0, 2), (1, 4))),
        "act_mask": with_ends((jax.random.randint(arg_keys[1], (M, NB), 0, 4) < 3).astype(jnp.int32), jax.random.fold_in(arg_keys[1], 1), 0, 1),
        "w1": normal_values(arg_keys[2], (NB, K, BS, BS), (K * BS) ** -0.5, 0.09375, ((0, 8), (1, 4))),
        "cols1": draw_cols1(jax.random.fold_in(arg_keys[9], 71), 0),
        "bias1": normal_values(arg_keys[4], (N,), 0.5, 3.0, ((0, 4),), jnp.float32),
        "mask2": with_ends((jax.random.randint(arg_keys[5], (M, NB), 0, 4) < 3).astype(jnp.int32), jax.random.fold_in(arg_keys[5], 1), 0, 1),
        "w2": normal_values(arg_keys[6], (NB, K, BS, BS), (K * BS // 4) ** -0.5, 0.1875, ((0, 8), (1, 4))),
        "cols2": draw_cols2(jax.random.fold_in(arg_keys[9], 71), 0),
        "bias2": normal_values(arg_keys[8], (N,), 0.5, 3.0, ((0, 16),), jnp.float32),
    }


def dense_layer(inputs, weights, targets, bias):
    blocks_in = inputs.reshape(M, NB, BS).astype(jnp.float32)

    def advance(running_total, block_row):
        incoming_rows = blocks_in[:, block_row]
        tiles = weights[block_row].astype(jnp.float32)
        product = jnp.einsum("mb,kbc->mkc", incoming_rows, tiles)
        return running_total.at[:, targets[block_row]].add(product), None

    start_value = jnp.zeros((M, NB, BS), jnp.float32)
    summed, unused = lax.scan(advance, start_value, jnp.arange(NB, dtype=jnp.int32))
    return jnp.maximum(summed + bias.reshape(NB, BS), 0.0)


def reference(acts, act_mask, w1, cols1, bias1, mask2, w2, cols2, bias2):
    masked = acts.reshape(M, NB, BS) * act_mask[:, :, None].astype(jnp.bfloat16)
    masked = masked.reshape(M, N)
    first = dense_layer(masked, w1, cols1, bias1)
    hidden = (first * mask2[:, :, None].astype(jnp.float32)).astype(jnp.bfloat16)
    second = dense_layer(hidden.reshape(M, N), w2, cols2, bias2)
    return second.astype(jnp.bfloat16).reshape(M, N)
```

```python
import functools

import jax
import jax.numpy as jnp
from jax import lax
from jax.experimental import pallas as pl
from jax.experimental.pallas import tpu as pltpu
from jax.sharding import PartitionSpec as P


def fold_function(inputs, targets, stride):

    def add_tiles(running_total, tiles, first_row):

        def advance(number, total):
            offset = number * stride
            block_list = lax.dynamic_slice_in_dim(tiles, offset, stride, 0)
            incoming_rows = lax.dynamic_slice_in_dim(inputs, offset, stride, 1)
            wanted = lax.dynamic_slice_in_dim(targets, offset, stride, 0)
            product = jnp.einsum(
                "tws,wish->twih", incoming_rows, block_list, preferred_element_type=jnp.float32
            )
            flat_product = product.reshape(product.shape[0], -1, product.shape[-1])
            return total.at[:, wanted.reshape(-1)].add(flat_product)

        return lax.fori_loop(0, tiles.shape[0] // stride, advance, running_total)

    return add_tiles


def gathered_weights(acts, act_mask, w1, cols1, bias1, mask2, w2, cols2, bias2):
    block = w1.shape[-1]
    rows_dev = acts.shape[0]
    row_blocks = act_mask.shape[1]
    col_blocks = mask2.shape[1]
    row_index = lax.axis_index("row")
    col_index = lax.axis_index("col")
    masked = acts.reshape(rows_dev, row_blocks, block) * act_mask[:, :, None].astype(jnp.bfloat16)
    first_layer_destinations = cols1 - col_index * col_blocks
    second_targets = cols2 - row_index * row_blocks
    first_offset_value = jnp.zeros((rows_dev, col_blocks, block), jnp.float32)
    first_fold = fold_function(masked, first_layer_destinations, w1.shape[0])
    first_sum = first_fold(
        first_offset_value, lax.all_gather(w1, "depth", axis=0, tiled=True), jnp.int32(0)
    )
    bias_blocks = bias1.reshape(col_blocks, block)
    share = col_blocks // lax.axis_size("row")
    part_sum = lax.psum_scatter(first_sum, "row", scatter_dimension=1, tiled=True)
    bias_part = lax.dynamic_slice_in_dim(bias_blocks, row_index * share, share, 0)
    mask_part = lax.dynamic_slice_in_dim(mask2, row_index * share, share, 1)
    hidden_part = jnp.maximum(part_sum + bias_part, 0.0) * mask_part[:, :, None].astype(jnp.float32)
    hidden = lax.all_gather(hidden_part.astype(jnp.bfloat16), "row", axis=1, tiled=True)
    second_start = jnp.zeros((rows_dev, row_blocks, block), jnp.float32)
    second_fold = fold_function(hidden, second_targets, w2.shape[0])
    second_sum = second_fold(
        second_start, lax.all_gather(w2, "depth", axis=0, tiled=True), jnp.int32(0)
    )
    outcome = lax.psum_scatter(second_sum, "col", scatter_dimension=1, tiled=True)
    bias_out = bias2.reshape(outcome.shape[1], block)
    return jnp.maximum(outcome + bias_out, 0.0).astype(jnp.bfloat16).reshape(rows_dev, -1)


MESH = pl.DeviceIdType.MESH
F32, BF16 = jnp.float32, jnp.bfloat16


def greet(partners):
    barrier = pltpu.get_barrier_semaphore()
    for partner in partners:
        pl.semaphore_signal(barrier, inc=1, device_id=partner, device_id_type=MESH)
    pl.semaphore_wait(barrier, len(partners))


def plan_rows(cols):
    stored, entries = cols.shape
    count = stored * entries
    small = cols.astype(BF16)

    def iota(shape, dim):
        return lax.broadcasted_iota(jnp.int32, shape, dim).astype(F32)

    def row_of(j):
        return jnp.floor((j + 0.5) * (1.0 / entries))

    lane = iota((entries, count), 1)
    spread = (lane - row_of(lane) * entries == iota((entries, count), 0)).astype(BF16)
    wide = jnp.dot(small, spread, preferred_element_type=F32)
    at = row_of(iota((stored, count), 1)) == iota((stored, count), 0)
    col_row = jnp.sum(jnp.where(at, wide, 0.0), axis=0, keepdims=True)
    down = (row_of(iota((count, stored), 0)) == iota((count, stored), 1)).astype(BF16)
    tall = jnp.dot(down, small, preferred_element_type=F32)
    line = iota((count, entries), 0)
    at = line - row_of(line) * entries == iota((count, entries), 1)
    col_col = jnp.sum(jnp.where(at, tall, 0.0), axis=1, keepdims=True)
    index_row, index_col = iota((1, count), 1), iota((count, 1), 0)
    key_row, key_col = col_row * count + index_row, col_col * count + index_col

    def total(flags, axis):
        return jnp.sum(jnp.where(flags, 1.0, 0.0), axis=axis, keepdims=True)

    rank = total(key_row < key_col, 1)
    less = total(col_row < col_col, 1)
    hit = rank == iota((count, count), 1)
    entry = jnp.sum(jnp.where(hit, index_col, 0.0), axis=0, keepdims=True)
    same = jnp.sum(jnp.where(hit, jnp.where(rank > less, 1.0, 0.0), 0.0), axis=0, keepdims=True)
    upto, below = total(col_col <= index_row, 0), total(col_col < index_row, 0)
    last = jnp.where(upto > below, upto - 1.0, float(count))
    return [row_of(entry), entry, same, last]


def prepare_kernel(acts, act_mask, cols1, cols2, mask2, staged, live_own, live_give, plan):
    r, c, d = lax.axis_index("row"), lax.axis_index("col"), lax.axis_index("depth")
    n_row = lax.axis_size("row")
    rows, row_blocks = act_mask.shape
    col_blocks = mask2.shape[1]
    block = staged.shape[-1]
    stored, size = row_blocks // 2, rows // 2
    mask = act_mask[...].astype(F32).astype(BF16)
    for b in range(row_blocks):
        where = (b // stored + d) % 2
        value = acts[:, b * block:(b + 1) * block] * mask[:, b:b + 1]
        for rc in range(2):
            staged[where, rc, b % stored] = value[rc * size:(rc + 1) * size]
    live = mask2[...].astype(F32).astype(BF16)
    share = col_blocks // 2 // n_row
    source = lax.broadcasted_iota(jnp.int32, (col_blocks, live_own.shape[1]), 0)
    target = lax.broadcasted_iota(jnp.int32, (col_blocks, live_own.shape[1]), 1)
    for ref, half in ((live_own, d), (live_give, 1 - d)):
        pick = (source == target + (half * (col_blocks // 2) + r * share)) & (target < share)
        pick = jnp.where(pick, 1.0, 0.0).astype(BF16)
        ref[...] = jnp.dot(live, pick, preferred_element_type=F32).astype(BF16)
    held = cols1.shape[0] // 2
    at = pl.ds(pl.multiple_of(d * held, 8), held)
    local1 = (cols1[at, :] - c * col_blocks).astype(F32)
    local2 = (cols2[at, :] - r * row_blocks).astype(F32)
    for n, value in enumerate(plan_rows(local1) + plan_rows(local2)):
        plan[n:n + 1, :] = value.astype(jnp.int32)


def prepare(acts, act_mask, cols1, cols2, mask2, block):
    rows, row_blocks = act_mask.shape
    count = cols1.shape[0] // 2 * cols1.shape[1]
    vmem = pl.BlockSpec(memory_space=pltpu.VMEM)
    return pl.pallas_call(
        prepare_kernel,
        out_shape=[
            jax.ShapeDtypeStruct((2, 2, row_blocks // 2, rows // 2, block), BF16),
            jax.ShapeDtypeStruct((rows, 128), BF16),
            jax.ShapeDtypeStruct((rows, 128), BF16),
            jax.ShapeDtypeStruct((8, count), jnp.int32),
        ],
        in_specs=[vmem] * 5,
        out_specs=[vmem] * 4,
        name="prepare",
    )(acts, act_mask, cols1, cols2, mask2)


def each(count, body, width=2):
    def step(at, carry):
        for u in range(width):
            body(at * width + u)
        return carry

    lax.fori_loop(0, count // width, step, 0)


def layers_kernel(
    n_col, plan, staged, live_own, live_give, bias1, bias2, w1, w2, out,
    wbuf, sums, acts_in0, acts_in1, live_in, kept, given, core_in, y_out, y_in, x_out, x_in,
    x1_00, x1_01, x1_10, x1_11, away, home, y2_in, z_out, z_in,
    load_sem, acts_send, acts_recv, live_sem, send_sem, recv_sem,
    send_y, recv_y, send_z, recv_z,
):
    r, c, d = lax.axis_index("row"), lax.axis_index("col"), lax.axis_index("depth")
    x, core = r // 2, r % 2
    partner = {"row": x * 2 + 1 - core}
    y_peer = {"depth": 1 - d}
    x_peer = {"row": (1 - x) * 2 + core}
    near = c % 2
    z_mate = {"col": c + 1 - 2 * near}
    entries, block = wbuf.shape[0], wbuf.shape[-1]
    size = sums.shape[1]
    share1 = bias1.shape[0]
    share2 = bias2.shape[0]
    acts_in = (acts_in0, acts_in1)
    x1 = ((x1_00, x1_01), (x1_10, x1_11))
    started = []

    def remote(source, target, send, recv, device):
        return pltpu.make_async_remote_copy(
            src_ref=source, dst_ref=target, send_sem=send, recv_sem=recv,
            device_id=device, device_id_type=MESH,
        )

    def begin(copy):
        copy.start()
        started.append(copy)

    def load(source, which):
        return pltpu.make_async_copy(source, wbuf, load_sem.at[which])

    load(w1, 0).start()
    greet([partner, y_peer, x_peer] + [{"col": lax.rem(c + o, n_col)} for o in range(1, n_col)])

    piece_blocks = acts_in0.shape[0] // 4

    def piece(which, part):
        return pl.ds((which * 2 + part) * piece_blocks, piece_blocks)

    for rc in range(2):
        for part in range(2):
            begin(remote(
                staged.at[1, rc, piece(near, part)], acts_in[rc].at[piece(near, part)],
                acts_send.at[0, rc, part], acts_recv.at[0, rc, part], y_peer,
            ))
    begin(remote(live_give, live_in, live_sem.at[0], live_sem.at[1], y_peer))

    def arrived(target, send, recv):
        remote(target, target, send, recv, y_peer).wait_recv()

    def pass_on(rc, part):
        mine = acts_in[rc].at[piece(near, part)]
        arrived(mine, acts_send.at[0, rc, part], acts_recv.at[0, rc, part])
        begin(remote(mine, mine, acts_send.at[1, rc, part], acts_recv.at[1, rc, part], z_mate))

    def passed(rc):
        for part in range(2):
            theirs = acts_in[rc].at[piece(1 - near, part)]
            arrived(theirs, acts_send.at[1, rc, part], acts_recv.at[1, rc, part])

    sums[entries] = jnp.zeros(sums.shape[1:], F32)

    def multiply(x_ref, layer):
        width = 16 if entries % 16 == 0 else 1

        def step(at, running):
            for u in range(width):
                p = at * width + u
                product = jnp.dot(
                    x_ref[plan[layer * 4, p]], wbuf[plan[layer * 4 + 1, p]],
                    preferred_element_type=F32,
                )
                running = running * plan[layer * 4 + 2, p].astype(F32) + product
                sums[p] = running
            return running

        lax.fori_loop(0, entries // width, step, jnp.zeros(sums.shape[1:], F32))

    def column(layer, b):
        return sums[plan[layer * 4 + 3, b]]

    def first_partial(h, rc):
        multiply(acts_in[rc] if h else staged.at[0, rc], 0)

        def split(q):
            at = (q // share1) * 2 * share1 + q % share1
            kept[h, rc, q] = column(0, at + core * share1)
            given[h, rc, q] = column(0, at + (1 - core) * share1).astype(BF16)

        each(kept.shape[2], split)
        send(0, given.at[h, rc], core_in.at[h, rc], h, rc, h, partner)

    def send(stage, source, target, h, rc, landing, device):
        begin(remote(
            source, target, send_sem.at[stage, h, rc], recv_sem.at[stage, landing, rc], device
        ))

    def await_stage(stage, target, h, rc):
        arrived(target, send_sem.at[stage, h, rc], recv_sem.at[stage, h, rc])

    half = kept.shape[2] // 2
    quarter = half // 2

    def pair(h, rc):
        await_stage(0, core_in.at[h, rc], h, rc)

        def other(q):
            at = (1 - d) * half + q
            y_out[h, rc, q] = (kept[h, rc, at] + core_in[h, rc, at].astype(F32)).astype(BF16)

        def own(q):
            at = d * half + q
            kept[h, rc, at] = kept[h, rc, at] + core_in[h, rc, at].astype(F32)

        each(half, other)
        send(1, y_out.at[h, rc], y_in.at[1 - h, rc], h, rc, 1 - h, y_peer)
        each(half, own)

    def along_y(h, rc):
        await_stage(1, y_in.at[h, rc], h, rc)

        def body(q):
            at = (1 - x) * quarter + q
            x_out[h, rc, q] = (
                kept[h, rc, d * half + at] + y_in[h, rc, at].astype(F32)
            ).astype(BF16)

        each(quarter, body)
        send(2, x_out.at[h, rc], x_in.at[h, rc], h, rc, h, x_peer)

    def slot(h, rc, row):
        return x1[h][rc].at[pl.ds(row * share1, share1)]

    def along_x(h, rc):
        await_stage(2, x_in.at[h, rc], h, rc)
        live = (live_in if h else live_own)[rc * size:(rc + 1) * size, :].astype(F32)
        for b in range(share1):
            at = x * quarter + b
            z = (
                kept[h, rc, d * half + at] + y_in[h, rc, at].astype(F32)
                + x_in[h, rc, b].astype(F32)
            )
            value = jnp.maximum(z + bias1[b:b + 1, :], 0.0) * live[:, b:b + 1]
            x1[h][rc][r * share1 + b] = value.astype(BF16)
        mine = slot(h, rc, r)
        send(3, mine, mine, h, rc, h, x_peer)
        send(4, mine, mine, h, rc, h, partner)

    def forward(h, rc):
        theirs = slot(h, rc, (1 - x) * 2 + core)
        await_stage(3, theirs, h, rc)
        send(5, theirs, theirs, h, rc, h, partner)

    def second_partial(h, rc):
        await_stage(4, slot(h, rc, x * 2 + 1 - core), h, rc)
        await_stage(5, slot(h, rc, (1 - x) * 2 + 1 - core), h, rc)
        multiply(x1[h][rc], 1)

        def body(b):
            if h:
                away[rc, b] = column(1, b).astype(BF16)
            else:
                home[rc, b] = column(1, b)

        each(home.shape[1], body)

    last = n_col - 1
    upper = c // 2
    inner = c + upper * (last - 2 * c)

    def mirrored(value):
        return value + upper * (last - 2 * value)

    def owner(i):
        end, mid = (3, 2, 1, 0)[i], (2, 0, 3, 1)[i]
        return mirrored(end + inner * (mid - end))

    def receiver(i):
        end, mid = (1, 2, 1)[i], (2, 0, 3)[i]
        return mirrored(end + inner * (mid - end))

    def y_copy(i, p):
        return remote(
            away.at[p, pl.ds(owner(i) * share2, share2)], y2_in.at[i, p],
            send_y.at[i, p], recv_y.at[i, p], y_peer,
        )

    def z_copy(i, p):
        at = 3 * inner if i == 0 else i
        return remote(
            z_out.at[i, p], z_in.at[at, p], send_z.at[i, p], recv_z.at[at, p],
            {"col": receiver(i)},
        )

    def z_arrival(at, p):
        remote(
            z_in.at[at, p], z_in.at[at, p], send_z.at[0, p], recv_z.at[at, p],
            {"col": receiver(0)},
        ).wait_recv()

    def near_sum(i, p, b):
        return home[p, owner(i) * share2 + b] + y2_in[i, p, b].astype(F32)

    def along_z(i, p):
        y_copy(i, p).wait_recv()

        def plain(b):
            z_out[i, p, b] = near_sum(i, p, b).astype(BF16)

        def joined(b):
            z_out[i, p, b] = (near_sum(i, p, b) + z_in[0, p, b].astype(F32)).astype(BF16)

        if i == 2:
            @pl.when(inner == 1)
            def _():
                z_arrival(0, p)
                each(share2, joined)

            @pl.when(inner == 0)
            def _():
                each(share2, plain)
        else:
            each(share2, plain)
        z_copy(i, p).start()

    def finish(p, slots):
        for at in slots:
            z_arrival(at, p)
        for b in range(share2):
            value = home[p, c * share2 + b] + y2_in[last, p, b].astype(F32)
            for at in slots:
                value += z_in[at, p, b].astype(F32)
            value = jnp.maximum(value + bias2[b:b + 1, :], 0.0)
            out[p * size:(p + 1) * size, b * block:(b + 1) * block] = value.astype(BF16)

    load(w1, 0).wait()
    first_partial(0, 0)
    pass_on(0, 0)
    first_partial(0, 1)
    pass_on(0, 1)
    pair(0, 0)
    pair(0, 1)
    pass_on(1, 0)
    pass_on(1, 1)
    passed(0)
    first_partial(1, 0)
    pair(1, 0)
    passed(1)
    first_partial(1, 1)
    load(w2, 1).start()
    arrived(live_in, live_sem.at[0], live_sem.at[1])
    along_y(1, 0)
    pair(1, 1)
    along_y(1, 1)
    along_x(1, 0)
    along_x(1, 1)
    forward(1, 0)
    along_y(0, 0)
    load(w2, 1).wait()
    second_partial(1, 0)
    y_copy(0, 0).start()
    forward(1, 1)
    along_x(0, 0)
    second_partial(1, 1)
    y_copy(0, 1).start()
    for i in range(1, n_col):
        for p in range(2):
            y_copy(i, p).start()
    along_y(0, 1)
    forward(0, 0)
    second_partial(0, 0)
    along_x(0, 1)
    along_z(0, 0)
    forward(0, 1)
    second_partial(0, 1)
    along_z(0, 1)
    for i in range(1, last):
        for p in range(2):
            along_z(i, p)
    for p in range(2):
        y_copy(last, p).wait_recv()

        @pl.when(inner == 1)
        def _():
            finish(p, (1, 2, 3))

        @pl.when(inner == 0)
        def _():
            finish(p, (1, 2))
    for copy in started:
        copy.wait_send()
    for i in range(n_col):
        for p in range(2):
            y_copy(i, p).wait_send()
            if i < last:
                z_copy(i, p).wait_send()


def fused_layers(acts, act_mask, w1, cols1, bias1, mask2, w2, cols2, bias2):
    block = w1.shape[-1]
    stored = w1.shape[0]
    rows = acts.shape[0]
    row_blocks, col_blocks = act_mask.shape[1], mask2.shape[1]
    n_row, n_col = lax.axis_size("row"), lax.axis_size("col")
    r, d = lax.axis_index("row"), lax.axis_index("depth")
    size = rows // 2
    share1 = col_blocks // 2 // n_row
    share2 = row_blocks // n_col
    staged, live_own, live_give, plan = prepare(acts, act_mask, cols1, cols2, mask2, block)
    first = d * (col_blocks // 2) + r * share1
    bias_part = lax.dynamic_slice_in_dim(bias1.reshape(col_blocks, block), first, share1, 0)
    flat1, flat2 = w1.reshape(-1, block, block), w2.reshape(-1, block, block)
    count = flat1.shape[0]
    half = col_blocks // 2
    smem = pl.BlockSpec(memory_space=pltpu.SMEM)
    vmem = pl.BlockSpec(memory_space=pltpu.VMEM)
    hbm = pl.BlockSpec(memory_space=pl.ANY)
    tile = (size, block)
    dma = pltpu.SemaphoreType.DMA
    return pl.pallas_call(
        functools.partial(layers_kernel, n_col),
        out_shape=jax.ShapeDtypeStruct((rows, share2 * block), BF16),
        in_specs=[smem] + [vmem] * 5 + [hbm] * 2,
        out_specs=vmem,
        scratch_shapes=[
            pltpu.VMEM((count, block, block), BF16),
            pltpu.VMEM((count + 1, *tile), F32),
            pltpu.VMEM((stored, *tile), BF16),
            pltpu.VMEM((stored, *tile), BF16),
            pltpu.VMEM((rows, 128), BF16),
            pltpu.VMEM((2, 2, half, *tile), F32),
            pltpu.VMEM((2, 2, half, *tile), BF16),
            pltpu.VMEM((2, 2, half, *tile), BF16),
            pltpu.VMEM((2, 2, half // 2, *tile), BF16),
            pltpu.VMEM((2, 2, half // 2, *tile), BF16),
            pltpu.VMEM((2, 2, share1, *tile), BF16),
            pltpu.VMEM((2, 2, share1, *tile), BF16),
            pltpu.VMEM((half, *tile), BF16),
            pltpu.VMEM((half, *tile), BF16),
            pltpu.VMEM((half, *tile), BF16),
            pltpu.VMEM((half, *tile), BF16),
            pltpu.VMEM((2, row_blocks, *tile), BF16),
            pltpu.VMEM((2, row_blocks, *tile), F32),
            pltpu.VMEM((n_col, 2, share2, *tile), BF16),
            pltpu.VMEM((n_col - 1, 2, share2, *tile), BF16),
            pltpu.VMEM((n_col, 2, share2, *tile), BF16),
            dma((2,)),
            dma((2, 2, 2)),
            dma((2, 2, 2)),
            dma((2,)),
            dma((6, 2, 2)),
            dma((6, 2, 2)),
            dma((n_col, 2)),
            dma((n_col, 2)),
            dma((n_col - 1, 2)),
            dma((n_col, 2)),
        ],
        compiler_params=pltpu.CompilerParams(
            collective_id=1, has_side_effects=True, vmem_limit_bytes=60 * 1024 * 1024
        ),
        name="layers",
    )(plan, staged, live_own, live_give, bias_part, bias2.reshape(share2, block), flat1, flat2)


def solution(mesh):
    near = mesh.shape["depth"] == 2 and mesh.shape["row"] == 4 and mesh.shape["col"] == 4
    return jax.shard_map(
        fused_layers if near else gathered_weights,
        mesh=mesh,
        in_specs=(
            P("depth", "row"),
            P("depth", "row"),
            P(("row", "depth"), "col", None, None),
            P("row", "col"),
            P("col"),
            P("depth", "col"),
            P(("col", "depth"), "row", None, None),
            P("col", "row"),
            P(("row", "col")),
        ),
        out_specs=P("depth", ("row", "col")),
        check_vma=False,
    )
```

```python
import functools

import jax
import jax.numpy as jnp
from jax import lax
from jax.experimental import pallas as pl
from jax.experimental.pallas import tpu as pltpu
from jax.sharding import PartitionSpec as P


def fold_function(inputs, targets, stride):

    def add_tiles(running_total, tiles, first_row):

        def advance(number, total):
            offset = number * stride
            block_list = lax.dynamic_slice_in_dim(tiles, offset, stride, 0)
            incoming_rows = lax.dynamic_slice_in_dim(inputs, offset, stride, 1)
            wanted = lax.dynamic_slice_in_dim(targets, offset, stride, 0)
            product = jnp.einsum(
                "tws,wish->twih", incoming_rows, block_list, preferred_element_type=jnp.float32
            )
            flat_product = product.reshape(product.shape[0], -1, product.shape[-1])
            return total.at[:, wanted.reshape(-1)].add(flat_product)

        return lax.fori_loop(0, tiles.shape[0] // stride, advance, running_total)

    return add_tiles


def gathered_weights(acts, act_mask, w1, cols1, bias1, mask2, w2, cols2, bias2):
    block = w1.shape[-1]
    rows_dev = acts.shape[0]
    row_blocks = act_mask.shape[1]
    col_blocks = mask2.shape[1]
    row_index = lax.axis_index("row")
    col_index = lax.axis_index("col")
    masked = acts.reshape(rows_dev, row_blocks, block) * act_mask[:, :, None].astype(jnp.bfloat16)
    first_layer_destinations = cols1 - col_index * col_blocks
    second_targets = cols2 - row_index * row_blocks
    first_offset_value = jnp.zeros((rows_dev, col_blocks, block), jnp.float32)
    first_fold = fold_function(masked, first_layer_destinations, w1.shape[0])
    first_sum = first_fold(
        first_offset_value, lax.all_gather(w1, "depth", axis=0, tiled=True), jnp.int32(0)
    )
    bias_blocks = bias1.reshape(col_blocks, block)
    share = col_blocks // lax.axis_size("row")
    part_sum = lax.psum_scatter(first_sum, "row", scatter_dimension=1, tiled=True)
    bias_part = lax.dynamic_slice_in_dim(bias_blocks, row_index * share, share, 0)
    mask_part = lax.dynamic_slice_in_dim(mask2, row_index * share, share, 1)
    hidden_part = jnp.maximum(part_sum + bias_part, 0.0) * mask_part[:, :, None].astype(jnp.float32)
    hidden = lax.all_gather(hidden_part.astype(jnp.bfloat16), "row", axis=1, tiled=True)
    second_start = jnp.zeros((rows_dev, row_blocks, block), jnp.float32)
    second_fold = fold_function(hidden, second_targets, w2.shape[0])
    second_sum = second_fold(
        second_start, lax.all_gather(w2, "depth", axis=0, tiled=True), jnp.int32(0)
    )
    outcome = lax.psum_scatter(second_sum, "col", scatter_dimension=1, tiled=True)
    bias_out = bias2.reshape(outcome.shape[1], block)
    return jnp.maximum(outcome + bias_out, 0.0).astype(jnp.bfloat16).reshape(rows_dev, -1)


MESH = pl.DeviceIdType.MESH
F32, BF16 = jnp.float32, jnp.bfloat16


def plan_rows(cols, first, stored):
    entries = cols.shape[0]
    count = stored * entries
    small = cols.astype(BF16)

    def iota(shape, dim):
        return lax.broadcasted_iota(jnp.int32, shape, dim).astype(F32)

    def row_of(j):
        return jnp.floor((j + 0.5) * (1.0 / entries))

    tall_shape = (cols.shape[1], count)
    spread = row_of(iota(tall_shape, 1)) + first.astype(F32) == iota(tall_shape, 0)
    spread = jnp.where(spread, 1.0, 0.0).astype(BF16)
    wide = jnp.dot(small, spread, preferred_element_type=F32)
    lane = iota((entries, count), 1)
    at = lane - row_of(lane) * entries == iota((entries, count), 0)
    col_row = jnp.sum(jnp.where(at, wide, 0.0), axis=0, keepdims=True)
    down_shape = (count, cols.shape[1])
    down = row_of(iota(down_shape, 0)) + first.astype(F32) == iota(down_shape, 1)
    down = jnp.where(down, 1.0, 0.0).astype(BF16)
    tall = lax.dot_general(down, small, (((1,), (1,)), ((), ())), preferred_element_type=F32)
    line = iota((count, entries), 0)
    at = line - row_of(line) * entries == iota((count, entries), 1)
    col_col = jnp.sum(jnp.where(at, tall, 0.0), axis=1, keepdims=True)
    index_row, index_col = iota((1, count), 1), iota((count, 1), 0)
    key_row, key_col = col_row * count + index_row, col_col * count + index_col

    def total(flags, axis):
        return jnp.sum(jnp.where(flags, 1.0, 0.0), axis=axis, keepdims=True)

    rank = total(key_row < key_col, 1)
    less = total(col_row < col_col, 1)
    hit = rank == iota((count, count), 1)
    entry = jnp.sum(jnp.where(hit, index_col, 0.0), axis=0, keepdims=True)
    same = jnp.sum(jnp.where(hit, jnp.where(rank > less, 1.0, 0.0), 0.0), axis=0, keepdims=True)
    upto, below = total(col_col <= index_row, 0), total(col_col < index_row, 0)
    last = jnp.where(upto > below, upto - 1.0, float(count))
    return [row_of(entry), entry, same, last]


def each(count, body, width=2):
    def step(at, carry):
        for u in range(width):
            body(at * width + u)
        return carry

    lax.fori_loop(0, count // width, step, 0)


def layers_kernel(
    n_col, fronts, acts, act_mask, cols1, cols2, mask2, bias1, bias2, w1, w2, out,
    wbuf, wbuf2, sums, acts_in0, acts_in1, keep_raw, give_raw, keep, give,
    act_mask_v, cols1_v, cols2_v, mask2_v, bias1_v, bias2_v, plan_v, plan, live_in,
    kept, given, core_in, y_out, y_in, x_out, x_in,
    x1_00, x1_01, x1_10, x1_11, away, home, y2_in, z_out, z_in,
    front, front_out, front_in, front_y_out, front_y_in,
    load_sem, acts_send, acts_recv, live_sem, send_sem, recv_sem,
    send_y, recv_y, send_z, recv_z, send_f, recv_f, send_fy, recv_fy,
):
    r, c, d = lax.axis_index("row"), lax.axis_index("col"), lax.axis_index("depth")
    n_row = lax.axis_size("row")
    x, core = r // 2, r % 2
    partner = {"row": x * 2 + 1 - core}
    y_peer = {"depth": 1 - d}
    x_peer = {"row": (1 - x) * 2 + core}
    near = c % 2
    z_mate = {"col": c + 1 - 2 * near}
    entries, block = wbuf.shape[0], wbuf.shape[-1]
    size = sums.shape[1]
    stored = acts_in0.shape[0]
    share1 = x_in.shape[2]
    share2 = bias2.shape[0]
    acts_in = (acts_in0, acts_in1)
    x1 = ((x1_00, x1_01), (x1_10, x1_11))
    started = []

    loads = []

    def load(source, target):
        copy = pltpu.make_async_copy(source, target, load_sem.at[len(loads)])
        copy.start()
        loads.append(copy)
        return copy

    half_blocks = stored // 2
    give_first = pl.multiple_of((1 - d) * stored + near * half_blocks, half_blocks)
    keep_first = pl.multiple_of(d * stored, stored)
    mask_loads = [load(act_mask, act_mask_v)]
    give_loads = [
        load(
            acts.at[pl.ds(rc * size, size), pl.ds(give_first * block, half_blocks * block)],
            give_raw.at[rc],
        )
        for rc in range(2)
    ]
    plan_loads = [load(cols1, cols1_v), load(cols2, cols2_v)]
    keep_loads = [
        load(
            acts.at[pl.ds(rc * size, size), pl.ds(keep_first * block, stored * block)],
            keep_raw.at[rc],
        )
        for rc in range(2)
    ]
    small_loads = [load(mask2, mask2_v), load(bias1, bias1_v), load(bias2, bias2_v)]
    w1_load = load(w1, wbuf)
    w2_load = load(w2, wbuf2)

    barrier = pltpu.get_barrier_semaphore()
    greeted = [partner, y_peer, x_peer]
    greeted += [{"col": lax.rem(c + o, n_col)} for o in range(1, n_col)]
    for device in greeted:
        pl.semaphore_signal(barrier, inc=1, device_id=device, device_id_type=MESH)

    def remote(source, target, send, recv, device):
        return pltpu.make_async_remote_copy(
            src_ref=source, dst_ref=target, send_sem=send, recv_sem=recv,
            device_id=device, device_id_type=MESH,
        )

    def begin(copy):
        copy.start()
        started.append(copy)

    parts = acts_send.shape[2]
    piece_blocks = half_blocks // parts

    def piece(which, part):
        return pl.ds(which * half_blocks + part * piece_blocks, piece_blocks)

    def mask_blocks(first, count):
        rows = act_mask_v[pl.ds(first, count), :]
        return rows.astype(F32).T.astype(BF16)

    def hand_over(rc, part):
        begin(remote(
            give.at[rc, pl.ds(part * piece_blocks, piece_blocks)],
            acts_in[rc].at[piece(near, part)],
            acts_send.at[0, rc, part], acts_recv.at[0, rc, part], y_peer,
        ))

    for copy in mask_loads:
        copy.wait()
    give_mask = mask_blocks(give_first, half_blocks)
    for rc in range(2):
        give_loads[rc].wait()
        for b in range(half_blocks):
            give[rc, b] = (
                give_raw[rc, :, b * block:(b + 1) * block]
                * give_mask[rc * size:(rc + 1) * size, b:b + 1]
            )
        if rc == 0:
            pl.semaphore_wait(barrier, len(greeted))
        for part in range(1 if rc else parts):
            hand_over(rc, part)
    for copy in plan_loads:
        copy.wait()
    held = cols1.shape[1] // 2
    local1 = plan_rows((cols1_v[...] - c * n_row * 2 * share1).astype(F32), d * held, held)
    local2 = plan_rows((cols2_v[...] - r * n_col * share2).astype(F32), d * held, held)
    for n, value in enumerate(local1 + local2):
        top = (stored - 1, entries - 1, 1, entries)[n % 4]
        plan_v[n:n + 1, :] = jnp.clip(value.astype(jnp.int32), 0, top)
    plan_copy = load(plan_v, plan)
    keep_mask = mask_blocks(keep_first, stored)
    for rc in range(2):
        keep_loads[rc].wait()
        for b in range(stored):
            keep[rc, b] = (
                keep_raw[rc, :, b * block:(b + 1) * block]
                * keep_mask[rc * size:(rc + 1) * size, b:b + 1]
            )
    for copy in small_loads:
        copy.wait()
    share_rows = n_row * share1

    def live_rows(side):
        return mask2_v.at[pl.ds(pl.multiple_of(side * share_rows + r * share1, share1), share1)]

    begin(remote(live_rows(1 - d), live_in, live_sem.at[0], live_sem.at[1], y_peer))
    plan_copy.wait()

    def arrived(target, send, recv):
        remote(target, target, send, recv, y_peer).wait_recv()

    def pass_on(rc, part):
        mine = acts_in[rc].at[piece(near, part)]
        arrived(mine, acts_send.at[0, rc, part], acts_recv.at[0, rc, part])
        begin(remote(mine, mine, acts_send.at[1, rc, part], acts_recv.at[1, rc, part], z_mate))

    def passed(rc):
        for part in range(parts):
            theirs = acts_in[rc].at[piece(1 - near, part)]
            arrived(theirs, acts_send.at[1, rc, part], acts_recv.at[1, rc, part])

    sums[entries] = jnp.zeros(sums.shape[1:], F32)

    def multiply(x_ref, layer):
        weights = wbuf2 if layer else wbuf
        width = 64 if entries % 64 == 0 else 1

        def step(at, running):
            for u in range(width):
                p = at * width + u
                product = jnp.dot(
                    x_ref[plan[layer * 4, p]], weights[plan[layer * 4 + 1, p]],
                    preferred_element_type=F32,
                )
                running = running * plan[layer * 4 + 2, p].astype(F32) + product
                sums[p] = running
            return running

        lax.fori_loop(0, entries // width, step, jnp.zeros(sums.shape[1:], F32))

    def column(layer, b):
        return sums[plan[layer * 4 + 3, b]]

    def first_partial(h, rc):
        multiply(acts_in[rc] if h else keep.at[rc], 0)

        def split(q):
            at = (q // share1) * 2 * share1 + q % share1
            kept[h, rc, q] = column(0, at + core * share1)
            given[h, rc, q] = column(0, at + (1 - core) * share1).astype(BF16)

        each(kept.shape[2], split)
        send(0, given.at[h, rc], core_in.at[h, rc], h, rc, h, partner)

    def send(stage, source, target, h, rc, landing, device):
        begin(remote(
            source, target, send_sem.at[stage, h, rc], recv_sem.at[stage, landing, rc], device
        ))

    def await_stage(stage, target, h, rc):
        arrived(target, send_sem.at[stage, h, rc], recv_sem.at[stage, h, rc])

    half = kept.shape[2] // 2
    quarter = half // 2

    def pair(h, rc):
        await_stage(0, core_in.at[h, rc], h, rc)

        def other(q):
            at = (1 - d) * half + q
            y_out[h, rc, q] = (kept[h, rc, at] + core_in[h, rc, at].astype(F32)).astype(BF16)

        def own(q):
            at = d * half + q
            kept[h, rc, at] = kept[h, rc, at] + core_in[h, rc, at].astype(F32)

        each(half, other)
        send(1, y_out.at[h, rc], y_in.at[1 - h, rc], h, rc, 1 - h, y_peer)
        each(half, own)

    def along_y(h, rc):
        await_stage(1, y_in.at[h, rc], h, rc)

        def body(q):
            at = (1 - x) * quarter + q
            x_out[h, rc, q] = (
                kept[h, rc, d * half + at] + y_in[h, rc, at].astype(F32)
            ).astype(BF16)

        each(quarter, body)
        send(2, x_out.at[h, rc], x_in.at[h, rc], h, rc, h, x_peer)

    def slot(h, rc, row):
        return x1[h][rc].at[pl.ds(row * share1, share1)]

    def along_x(h, rc):
        await_stage(2, x_in.at[h, rc], h, rc)
        live = (live_in if h else live_rows(d))[...].astype(F32).T[rc * size:(rc + 1) * size]
        shift = bias1_v[pl.ds(pl.multiple_of((d * n_row + r) * share1, share1), share1), :]
        for b in range(share1):
            at = x * quarter + b
            z = (
                kept[h, rc, d * half + at] + y_in[h, rc, at].astype(F32)
                + x_in[h, rc, b].astype(F32)
            )
            value = jnp.maximum(z + shift[b:b + 1, :], 0.0) * live[:, b:b + 1]
            x1[h][rc][r * share1 + b] = value.astype(BF16)
        mine = slot(h, rc, r)
        send(3, mine, mine, h, rc, h, x_peer)
        send(4, mine, mine, h, rc, h, partner)

    def forward(h, rc):
        theirs = slot(h, rc, (1 - x) * 2 + core)
        await_stage(3, theirs, h, rc)
        send(5, theirs, theirs, h, rc, h, partner)

    def second_partial(h, rc):
        await_stage(4, slot(h, rc, x * 2 + 1 - core), h, rc)
        await_stage(5, slot(h, rc, (1 - x) * 2 + 1 - core), h, rc)
        multiply(x1[h][rc], 1)

        def body(b):
            if h:
                away[rc, b] = column(1, b).astype(BF16)
            else:
                home[rc, b] = column(1, b)

        each(home.shape[1], body)

        def ahead(q):
            front[h, rc, q] = column(1, (q // fronts) * share2 + main2 + q % fronts)

        each(n_col * fronts, ahead)

    main2 = share2 - fronts
    last = n_col - 1
    upper = c // 2
    inner = c + upper * (last - 2 * c)

    def mirrored(value):
        return value + upper * (last - 2 * value)

    def owner(i):
        end, mid = (3, 2, 1, 0)[i], (2, 0, 3, 1)[i]
        return mirrored(end + inner * (mid - end))

    def receiver(i):
        end, mid = (1, 2, 1)[i], (2, 0, 3)[i]
        return mirrored(end + inner * (mid - end))

    def y_copy(i, p):
        return remote(
            away.at[p, pl.ds(owner(i) * share2, main2)], y2_in.at[i, p],
            send_y.at[i, p], recv_y.at[i, p], y_peer,
        )

    def z_copy(i, p):
        at = 3 * inner if i == 0 else i
        return remote(
            z_out.at[i, p], z_in.at[at, p], send_z.at[i, p], recv_z.at[at, p],
            {"col": receiver(i)},
        )

    def z_arrival(at, p):
        remote(
            z_in.at[at, p], z_in.at[at, p], send_z.at[0, p], recv_z.at[at, p],
            {"col": receiver(0)},
        ).wait_recv()

    def near_sum(i, p, b):
        return home[p, owner(i) * share2 + b] + y2_in[i, p, b].astype(F32)

    def along_z(i, p):
        y_copy(i, p).wait_recv()

        def plain(b):
            z_out[i, p, b] = near_sum(i, p, b).astype(BF16)

        def joined(b):
            z_out[i, p, b] = (near_sum(i, p, b) + z_in[0, p, b].astype(F32)).astype(BF16)

        if i == 2:
            @pl.when(inner == 1)
            def _():
                z_arrival(0, p)
                each(main2, joined)

            @pl.when(inner == 0)
            def _():
                each(main2, plain)
        else:
            each(main2, plain)
        z_copy(i, p).start()

    def front_copy(i, h, p):
        at = 3 * inner if i == 0 else i
        return remote(
            front_out.at[i, h, p], front_in.at[at, h, p],
            send_f.at[i, h, p], recv_f.at[at, h, p], {"col": receiver(i)},
        )

    def front_arrival(at, h, p):
        remote(
            front_in.at[at, h, p], front_in.at[at, h, p],
            send_f.at[0, h, p], recv_f.at[at, h, p], {"col": receiver(0)},
        ).wait_recv()

    def front_send(i, h, p):
        def put(with_arrival):
            for b in range(fronts):
                value = front[h, p, owner(i) * fronts + b]
                if with_arrival:
                    value += front_in[0, h, p, b].astype(F32)
                front_out[i, h, p, b] = value.astype(BF16)

        if i == 2:
            @pl.when(inner == 1)
            def _():
                front_arrival(0, h, p)
                put(True)

            @pl.when(inner == 0)
            def _():
                put(False)
        else:
            put(False)
        front_copy(i, h, p).start()

    def front_total(h, p, slots):
        for at in slots:
            front_arrival(at, h, p)
        for b in range(fronts):
            value = front[h, p, c * fronts + b]
            for at in slots:
                value += front_in[at, h, p, b].astype(F32)
            if h:
                front_y_out[p, b] = value.astype(BF16)
            else:
                front[h, p, c * fronts + b] = value

    def by_place(work):
        @pl.when(inner == 1)
        def _():
            work((1, 2, 3))

        @pl.when(inner == 0)
        def _():
            work((1, 2))

    def front_close(h, p):
        by_place(functools.partial(front_total, h, p))
        if h:
            begin(remote(
                front_y_out.at[p], front_y_in.at[p], send_fy.at[p], recv_fy.at[p], y_peer
            ))

    def put_out(p, b, value):
        value = jnp.maximum(value + bias2_v[b:b + 1, :], 0.0)
        out[p * size:(p + 1) * size, b * block:(b + 1) * block] = value.astype(BF16)

    def front_finish(p):
        arrived(front_y_in.at[p], send_fy.at[p], recv_fy.at[p])
        for b in range(fronts):
            put_out(p, main2 + b, front[0, p, c * fronts + b] + front_y_in[p, b].astype(F32))

    def finish(p, slots):
        for at in slots:
            z_arrival(at, p)
        for b in range(main2):
            value = home[p, c * share2 + b] + y2_in[last, p, b].astype(F32)
            for at in slots:
                value += z_in[at, p, b].astype(F32)
            put_out(p, b, value)

    def finish_wait(p):
        y_copy(last, p).wait_recv()

    w1_load.wait()
    first_partial(0, 0)
    pass_on(0, 0)
    pair(0, 0)
    for part in range(1, parts):
        hand_over(1, part)
    for part in range(1, parts):
        pass_on(0, part)
    first_partial(0, 1)
    pass_on(1, 0)
    passed(0)
    first_partial(1, 0)
    pair(1, 0)
    along_y(1, 0)
    pair(0, 1)
    for part in range(1, parts):
        pass_on(1, part)
    arrived(live_in, live_sem.at[0], live_sem.at[1])
    along_x(1, 0)
    passed(1)
    first_partial(1, 1)
    along_y(0, 0)
    forward(1, 0)
    pair(1, 1)
    w2_load.wait()
    second_partial(1, 0)
    for i in range(n_col):
        y_copy(i, 0).start()
    front_send(0, 1, 0)
    front_send(1, 1, 0)
    along_x(0, 0)
    along_y(1, 1)
    along_y(0, 1)
    forward(0, 0)
    second_partial(0, 0)
    along_x(1, 1)
    along_z(0, 0)
    front_send(0, 0, 0)
    front_send(1, 0, 0)
    along_x(0, 1)
    front_send(2, 1, 0)
    along_z(1, 0)
    forward(1, 1)
    second_partial(1, 1)
    for i in range(n_col):
        y_copy(i, 1).start()
    along_z(2, 0)
    front_send(0, 1, 1)
    front_send(1, 1, 1)
    front_send(2, 0, 0)
    forward(0, 1)
    second_partial(0, 1)
    front_send(0, 0, 1)
    front_send(1, 0, 1)
    along_z(0, 1)
    front_send(2, 1, 1)
    front_send(2, 0, 1)
    front_close(1, 0)
    along_z(1, 1)
    finish_wait(0)
    by_place(functools.partial(finish, 0))
    front_close(1, 1)
    front_close(0, 0)
    along_z(2, 1)
    front_close(0, 1)
    front_finish(0)
    finish_wait(1)
    by_place(functools.partial(finish, 1))
    front_finish(1)
    for copy in started:
        copy.wait_send()
    for i in range(n_col):
        for p in range(2):
            y_copy(i, p).wait_send()
            if i < last:
                z_copy(i, p).wait_send()
                front_copy(i, 0, p).wait_send()
                front_copy(i, 1, p).wait_send()


def fused_layers(acts, act_mask, w1, cols1, bias1, mask2, w2, cols2, bias2):
    block = w1.shape[-1]
    stored = w1.shape[0]
    rows = acts.shape[0]
    row_blocks, col_blocks = act_mask.shape[1], mask2.shape[1]
    n_row, n_col = lax.axis_size("row"), lax.axis_size("col")
    size = rows // 2
    share1 = col_blocks // 2 // n_row
    share2 = row_blocks // n_col
    fronts = share2 // 8
    flat1, flat2 = w1.reshape(-1, block, block), w2.reshape(-1, block, block)
    count = flat1.shape[0]
    half = col_blocks // 2
    parts = 4
    vmem = pl.BlockSpec(memory_space=pltpu.VMEM)
    hbm = pl.BlockSpec(memory_space=pltpu.HBM)
    tile = (size, block)
    dma = pltpu.SemaphoreType.DMA
    return pl.pallas_call(
        functools.partial(layers_kernel, n_col, fronts),
        out_shape=jax.ShapeDtypeStruct((rows, share2 * block), BF16),
        in_specs=[hbm] * 9,
        out_specs=vmem,
        scratch_shapes=[
            pltpu.VMEM((count, block, block), BF16),
            pltpu.VMEM((count, block, block), BF16),
            pltpu.VMEM((count + 1, *tile), F32),
            pltpu.VMEM((stored, *tile), BF16),
            pltpu.VMEM((stored, *tile), BF16),
            pltpu.VMEM((2, size, stored * block), BF16),
            pltpu.VMEM((2, size, stored // 2 * block), BF16),
            pltpu.VMEM((2, stored, *tile), BF16),
            pltpu.VMEM((2, stored // 2, *tile), BF16),
            pltpu.VMEM((row_blocks, rows), jnp.int32),
            pltpu.VMEM(cols1.shape[::-1], jnp.int32),
            pltpu.VMEM(cols2.shape[::-1], jnp.int32),
            pltpu.VMEM((col_blocks, rows), jnp.int32),
            pltpu.VMEM((col_blocks, block), F32),
            pltpu.VMEM((share2, block), F32),
            pltpu.VMEM((8, count), jnp.int32),
            pltpu.SMEM((8, count), jnp.int32),
            pltpu.VMEM((share1, rows), jnp.int32),
            pltpu.VMEM((2, 2, half, *tile), F32),
            pltpu.VMEM((2, 2, half, *tile), BF16),
            pltpu.VMEM((2, 2, half, *tile), BF16),
            pltpu.VMEM((2, 2, half // 2, *tile), BF16),
            pltpu.VMEM((2, 2, half // 2, *tile), BF16),
            pltpu.VMEM((2, 2, share1, *tile), BF16),
            pltpu.VMEM((2, 2, share1, *tile), BF16),
            pltpu.VMEM((half, *tile), BF16),
            pltpu.VMEM((half, *tile), BF16),
            pltpu.VMEM((half, *tile), BF16),
            pltpu.VMEM((half, *tile), BF16),
            pltpu.VMEM((2, row_blocks, *tile), BF16),
            pltpu.VMEM((2, row_blocks, *tile), F32),
            pltpu.VMEM((n_col, 2, share2 - fronts, *tile), BF16),
            pltpu.VMEM((n_col - 1, 2, share2 - fronts, *tile), BF16),
            pltpu.VMEM((n_col, 2, share2 - fronts, *tile), BF16),
            pltpu.VMEM((2, 2, n_col * fronts, *tile), F32),
            pltpu.VMEM((n_col - 1, 2, 2, fronts, *tile), BF16),
            pltpu.VMEM((n_col, 2, 2, fronts, *tile), BF16),
            pltpu.VMEM((2, fronts, *tile), BF16),
            pltpu.VMEM((2, fronts, *tile), BF16),
            dma((16,)),
            dma((2, 2, parts)),
            dma((2, 2, parts)),
            dma((2,)),
            dma((6, 2, 2)),
            dma((6, 2, 2)),
            dma((n_col, 2)),
            dma((n_col, 2)),
            dma((n_col - 1, 2)),
            dma((n_col, 2)),
            dma((n_col - 1, 2, 2)),
            dma((n_col, 2, 2)),
            dma((2,)),
            dma((2,)),
        ],
        compiler_params=pltpu.CompilerParams(
            collective_id=1, has_side_effects=True, vmem_limit_bytes=62 * 1024 * 1024
        ),
        name="layers",
    )(
        acts, act_mask.T, cols1.T, cols2.T, mask2.T, bias1.reshape(col_blocks, block),
        bias2.reshape(share2, block), flat1, flat2,
    )


def solution(mesh):
    near = mesh.shape["depth"] == 2 and mesh.shape["row"] == 4 and mesh.shape["col"] == 4
    return jax.shard_map(
        fused_layers if near else gathered_weights,
        mesh=mesh,
        in_specs=(
            P("depth", "row"),
            P("depth", "row"),
            P(("row", "depth"), "col", None, None),
            P("row", "col"),
            P("col"),
            P("depth", "col"),
            P(("col", "depth"), "row", None, None),
            P("col", "row"),
            P(("row", "col")),
        ),
        out_specs=P("depth", ("row", "col")),
        check_vma=False,
    )
```

```python
import functools

import jax
import jax.numpy as jnp
from jax import lax
from jax.experimental import pallas as pl
from jax.experimental.pallas import tpu as pltpu
from jax.sharding import PartitionSpec as P


def fold_function(inputs, targets, stride):

    def add_tiles(running_total, tiles, first_row):

        def advance(number, total):
            offset = number * stride
            block_list = lax.dynamic_slice_in_dim(tiles, offset, stride, 0)
            incoming_rows = lax.dynamic_slice_in_dim(inputs, offset, stride, 1)
            wanted = lax.dynamic_slice_in_dim(targets, offset, stride, 0)
            product = jnp.einsum(
                "tws,wish->twih", incoming_rows, block_list, preferred_element_type=jnp.float32
            )
            flat_product = product.reshape(product.shape[0], -1, product.shape[-1])
            return total.at[:, wanted.reshape(-1)].add(flat_product)

        return lax.fori_loop(0, tiles.shape[0] // stride, advance, running_total)

    return add_tiles


def gathered_weights(acts, act_mask, w1, cols1, bias1, mask2, w2, cols2, bias2):
    block = w1.shape[-1]
    rows_dev = acts.shape[0]
    row_blocks = act_mask.shape[1]
    col_blocks = mask2.shape[1]
    row_index = lax.axis_index("row")
    col_index = lax.axis_index("col")
    masked = acts.reshape(rows_dev, row_blocks, block) * act_mask[:, :, None].astype(jnp.bfloat16)
    first_layer_destinations = cols1 - col_index * col_blocks
    second_targets = cols2 - row_index * row_blocks
    first_offset_value = jnp.zeros((rows_dev, col_blocks, block), jnp.float32)
    first_fold = fold_function(masked, first_layer_destinations, w1.shape[0])
    first_sum = first_fold(
        first_offset_value, lax.all_gather(w1, "depth", axis=0, tiled=True), jnp.int32(0)
    )
    bias_blocks = bias1.reshape(col_blocks, block)
    share = col_blocks // lax.axis_size("row")
    part_sum = lax.psum_scatter(first_sum, "row", scatter_dimension=1, tiled=True)
    bias_part = lax.dynamic_slice_in_dim(bias_blocks, row_index * share, share, 0)
    mask_part = lax.dynamic_slice_in_dim(mask2, row_index * share, share, 1)
    hidden_part = jnp.maximum(part_sum + bias_part, 0.0) * mask_part[:, :, None].astype(jnp.float32)
    hidden = lax.all_gather(hidden_part.astype(jnp.bfloat16), "row", axis=1, tiled=True)
    second_start = jnp.zeros((rows_dev, row_blocks, block), jnp.float32)
    second_fold = fold_function(hidden, second_targets, w2.shape[0])
    second_sum = second_fold(
        second_start, lax.all_gather(w2, "depth", axis=0, tiled=True), jnp.int32(0)
    )
    outcome = lax.psum_scatter(second_sum, "col", scatter_dimension=1, tiled=True)
    bias_out = bias2.reshape(outcome.shape[1], block)
    return jnp.maximum(outcome + bias_out, 0.0).astype(jnp.bfloat16).reshape(rows_dev, -1)


MESH = pl.DeviceIdType.MESH
F32, BF16 = jnp.float32, jnp.bfloat16


def plan_rows(cols, first, stored):
    entries = cols.shape[0]
    count = stored * entries
    small = cols.astype(BF16)

    def iota(shape, dim):
        return lax.broadcasted_iota(jnp.int32, shape, dim).astype(F32)

    def row_of(j):
        return jnp.floor((j + 0.5) * (1.0 / entries))

    tall_shape = (cols.shape[1], count)
    spread = row_of(iota(tall_shape, 1)) + first.astype(F32) == iota(tall_shape, 0)
    spread = jnp.where(spread, 1.0, 0.0).astype(BF16)
    wide = jnp.dot(small, spread, preferred_element_type=F32)
    lane = iota((entries, count), 1)
    at = lane - row_of(lane) * entries == iota((entries, count), 0)
    col_row = jnp.sum(jnp.where(at, wide, 0.0), axis=0, keepdims=True)
    down_shape = (count, cols.shape[1])
    down = row_of(iota(down_shape, 0)) + first.astype(F32) == iota(down_shape, 1)
    down = jnp.where(down, 1.0, 0.0).astype(BF16)
    tall = lax.dot_general(down, small, (((1,), (1,)), ((), ())), preferred_element_type=F32)
    line = iota((count, entries), 0)
    at = line - row_of(line) * entries == iota((count, entries), 1)
    col_col = jnp.sum(jnp.where(at, tall, 0.0), axis=1, keepdims=True)
    index_row, index_col = iota((1, count), 1), iota((count, 1), 0)
    key_row, key_col = col_row * count + index_row, col_col * count + index_col

    def total(flags, axis):
        return jnp.sum(jnp.where(flags, 1.0, 0.0), axis=axis, keepdims=True)

    rank = total(key_row < key_col, 1)
    less = total(col_row < col_col, 1)
    hit = rank == iota((count, count), 1)
    entry = jnp.sum(jnp.where(hit, index_col, 0.0), axis=0, keepdims=True)
    same = jnp.sum(jnp.where(hit, jnp.where(rank > less, 1.0, 0.0), 0.0), axis=0, keepdims=True)
    upto, below = total(col_col <= index_row, 0), total(col_col < index_row, 0)
    last = jnp.where(upto > below, upto - 1.0, float(count))
    return [row_of(entry), entry, same, last]


def each(count, body, width=2):
    def step(at, carry):
        for u in range(width):
            body(at * width + u)
        return carry

    lax.fori_loop(0, count // width, step, 0)


def layers_kernel(
    n_col, fronts, acts, act_mask, cols1, cols2, mask2, bias1, bias2, w1, w2, out,
    wbuf, wbuf2, sums, acts_in0, acts_in1, keep_raw, give_raw, keep, give,
    act_mask_v, cols1_v, cols2_v, mask2_v, bias1_v, bias2_v, plan_v, plan, live_in,
    kept, given, core_in, y_out, y_in, x_out, x_in,
    x1_00, x1_01, x1_10, x1_11, away, home, y2_in, z_out, z_in,
    front, front_out, front_in, front_y_out, front_y_in,
    load_sem, acts_send, acts_recv, live_sem, send_sem, recv_sem,
    send_y, recv_y, send_z, recv_z, send_f, recv_f, send_fy, recv_fy,
):
    r, c, d = lax.axis_index("row"), lax.axis_index("col"), lax.axis_index("depth")
    n_row = lax.axis_size("row")
    x, core = r // 2, r % 2
    partner = {"row": x * 2 + 1 - core}
    y_peer = {"depth": 1 - d}
    x_peer = {"row": (1 - x) * 2 + core}
    near = c % 2
    z_mate = {"col": c + 1 - 2 * near}
    entries, block = wbuf.shape[0], wbuf.shape[-1]
    size = sums.shape[1]
    stored = acts_in0.shape[0]
    share1 = x_in.shape[2]
    share2 = bias2.shape[0]
    acts_in = (acts_in0, acts_in1)
    x1 = ((x1_00, x1_01), (x1_10, x1_11))
    started = []

    loads = []

    def load(source, target):
        copy = pltpu.make_async_copy(source, target, load_sem.at[len(loads)])
        copy.start()
        loads.append(copy)
        return copy

    half_blocks = stored // 2
    give_first = pl.multiple_of((1 - d) * stored + near * half_blocks, half_blocks)
    keep_first = pl.multiple_of(d * stored, stored)
    mask_loads = [load(act_mask, act_mask_v)]
    give_loads = [
        load(
            acts.at[pl.ds(rc * size, size), pl.ds(give_first * block, half_blocks * block)],
            give_raw.at[rc],
        )
        for rc in range(2)
    ]
    plan_loads = [load(cols1, cols1_v), load(cols2, cols2_v)]
    keep_loads = [
        load(
            acts.at[pl.ds(rc * size, size), pl.ds(keep_first * block, stored * block)],
            keep_raw.at[rc],
        )
        for rc in range(2)
    ]
    small_loads = [load(mask2, mask2_v), load(bias1, bias1_v), load(bias2, bias2_v)]
    w1_load = load(w1, wbuf)
    w2_load = load(w2, wbuf2)

    barrier = pltpu.get_barrier_semaphore()
    greeted = [partner, y_peer, x_peer]
    greeted += [{"col": lax.rem(c + o, n_col)} for o in range(1, n_col)]
    for device in greeted:
        pl.semaphore_signal(barrier, inc=1, device_id=device, device_id_type=MESH)

    def remote(source, target, send, recv, device):
        return pltpu.make_async_remote_copy(
            src_ref=source, dst_ref=target, send_sem=send, recv_sem=recv,
            device_id=device, device_id_type=MESH,
        )

    def begin(copy):
        copy.start()
        started.append(copy)

    parts = acts_send.shape[2]
    piece_blocks = half_blocks // parts

    def piece(which, part):
        return pl.ds(which * half_blocks + part * piece_blocks, piece_blocks)

    def mask_blocks(first, count):
        rows = act_mask_v[pl.ds(first, count), :]
        return rows.astype(F32).T.astype(BF16)

    def hand_over(rc, part):
        begin(remote(
            give.at[rc, pl.ds(part * piece_blocks, piece_blocks)],
            acts_in[rc].at[piece(near, part)],
            acts_send.at[0, rc, part], acts_recv.at[0, rc, part], y_peer,
        ))

    for copy in mask_loads:
        copy.wait()
    give_mask = mask_blocks(give_first, half_blocks)
    for rc in range(2):
        give_loads[rc].wait()
        for b in range(half_blocks):
            give[rc, b] = (
                give_raw[rc, :, b * block:(b + 1) * block]
                * give_mask[rc * size:(rc + 1) * size, b:b + 1]
            )
        if rc == 0:
            pl.semaphore_wait(barrier, len(greeted))
        for part in range(1 if rc else parts):
            hand_over(rc, part)
    for copy in plan_loads:
        copy.wait()
    held = cols1.shape[1] // 2
    local1 = plan_rows((cols1_v[...] - c * n_row * 2 * share1).astype(F32), d * held, held)
    local2 = plan_rows((cols2_v[...] - r * n_col * share2).astype(F32), d * held, held)
    for n, value in enumerate(local1 + local2):
        top = (stored - 1, entries - 1, 1, entries)[n % 4]
        plan_v[n:n + 1, :] = jnp.clip(value.astype(jnp.int32), 0, top)
    plan_copy = load(plan_v, plan)
    keep_mask = mask_blocks(keep_first, stored)
    for rc in range(2):
        keep_loads[rc].wait()
        for b in range(stored):
            keep[rc, b] = (
                keep_raw[rc, :, b * block:(b + 1) * block]
                * keep_mask[rc * size:(rc + 1) * size, b:b + 1]
            )
    for copy in small_loads:
        copy.wait()
    share_rows = n_row * share1

    def live_rows(side):
        return mask2_v.at[pl.ds(pl.multiple_of(side * share_rows + r * share1, share1), share1)]

    begin(remote(live_rows(1 - d), live_in, live_sem.at[0], live_sem.at[1], y_peer))
    plan_copy.wait()

    def arrived(target, send, recv):
        remote(target, target, send, recv, y_peer).wait_recv()

    def pass_on(rc, part):
        mine = acts_in[rc].at[piece(near, part)]
        arrived(mine, acts_send.at[0, rc, part], acts_recv.at[0, rc, part])
        begin(remote(mine, mine, acts_send.at[1, rc, part], acts_recv.at[1, rc, part], z_mate))

    def passed(rc):
        for part in range(parts):
            theirs = acts_in[rc].at[piece(1 - near, part)]
            arrived(theirs, acts_send.at[1, rc, part], acts_recv.at[1, rc, part])

    sums[entries] = jnp.zeros(sums.shape[1:], F32)

    def multiply(x_ref, layer, between):
        weights = wbuf2 if layer else wbuf
        width = 64 if entries % 64 == 0 else 1

        def step(at, running):
            for u in range(width):
                p = at * width + u
                product = jnp.dot(
                    x_ref[plan[layer * 4, p]], weights[plan[layer * 4 + 1, p]],
                    preferred_element_type=F32,
                )
                running = running * plan[layer * 4 + 2, p].astype(F32) + product
                sums[p] = running
            return running

        steps = entries // width
        running = lax.fori_loop(0, steps // 2, step, jnp.zeros(sums.shape[1:], F32))
        if between is not None:
            between()
        lax.fori_loop(steps // 2, steps, step, running)

    def column(layer, b):
        return sums[plan[layer * 4 + 3, b]]

    def first_partial(h, rc, between=None):
        multiply(acts_in[rc] if h else keep.at[rc], 0, between)

        def split(q):
            at = (q // share1) * 2 * share1 + q % share1
            kept[h, rc, q] = column(0, at + core * share1)
            given[h, rc, q] = column(0, at + (1 - core) * share1).astype(BF16)

        each(kept.shape[2], split)
        send(0, given.at[h, rc], core_in.at[h, rc], h, rc, h, partner)

    def send(stage, source, target, h, rc, landing, device):
        begin(remote(
            source, target, send_sem.at[stage, h, rc], recv_sem.at[stage, landing, rc], device
        ))

    def await_stage(stage, target, h, rc):
        arrived(target, send_sem.at[stage, h, rc], recv_sem.at[stage, h, rc])

    half = kept.shape[2] // 2
    quarter = half // 2

    def pair(h, rc):
        await_stage(0, core_in.at[h, rc], h, rc)

        def other(q):
            at = (1 - d) * half + q
            y_out[h, rc, q] = (kept[h, rc, at] + core_in[h, rc, at].astype(F32)).astype(BF16)

        def own(q):
            at = d * half + q
            kept[h, rc, at] = kept[h, rc, at] + core_in[h, rc, at].astype(F32)

        each(half, other)
        send(1, y_out.at[h, rc], y_in.at[1 - h, rc], h, rc, 1 - h, y_peer)
        each(half, own)

    def along_y(h, rc):
        await_stage(1, y_in.at[h, rc], h, rc)

        def body(q):
            at = (1 - x) * quarter + q
            x_out[h, rc, q] = (
                kept[h, rc, d * half + at] + y_in[h, rc, at].astype(F32)
            ).astype(BF16)

        each(quarter, body)
        send(2, x_out.at[h, rc], x_in.at[h, rc], h, rc, h, x_peer)

    def slot(h, rc, row):
        return x1[h][rc].at[pl.ds(row * share1, share1)]

    def along_x(h, rc):
        await_stage(2, x_in.at[h, rc], h, rc)
        live = (live_in if h else live_rows(d))[...].astype(F32).T[rc * size:(rc + 1) * size]
        shift = bias1_v[pl.ds(pl.multiple_of((d * n_row + r) * share1, share1), share1), :]
        for b in range(share1):
            at = x * quarter + b
            z = (
                kept[h, rc, d * half + at] + y_in[h, rc, at].astype(F32)
                + x_in[h, rc, b].astype(F32)
            )
            value = jnp.maximum(z + shift[b:b + 1, :], 0.0) * live[:, b:b + 1]
            x1[h][rc][r * share1 + b] = value.astype(BF16)
        mine = slot(h, rc, r)
        send(3, mine, mine, h, rc, h, x_peer)
        send(4, mine, mine, h, rc, h, partner)

    def forward(h, rc):
        theirs = slot(h, rc, (1 - x) * 2 + core)
        await_stage(3, theirs, h, rc)
        send(5, theirs, theirs, h, rc, h, partner)

    def second_partial(h, rc, between=None):
        await_stage(4, slot(h, rc, x * 2 + 1 - core), h, rc)
        await_stage(5, slot(h, rc, (1 - x) * 2 + 1 - core), h, rc)
        multiply(x1[h][rc], 1, between)

        def body(b):
            if h:
                away[rc, b] = column(1, b).astype(BF16)
            else:
                home[rc, b] = column(1, b)

        each(home.shape[1], body)

        def ahead(q):
            front[h, q] = column(1, (q // fronts) * share2 + mains[0] + q % fronts)

        if rc == 0:
            each(n_col * fronts, ahead)

    mains = (share2 - fronts, share2)

    def main(ref, i, p):
        return ref.at[i, p, pl.ds(0, mains[p])]

    last = n_col - 1
    upper = c // 2
    inner = c + upper * (last - 2 * c)

    def mirrored(value):
        return value + upper * (last - 2 * value)

    def owner(i):
        end, mid = (3, 2, 1, 0)[i], (2, 0, 3, 1)[i]
        return mirrored(end + inner * (mid - end))

    def receiver(i):
        end, mid = (1, 2, 1)[i], (2, 0, 3)[i]
        return mirrored(end + inner * (mid - end))

    def y_copy(i, p):
        return remote(
            away.at[p, pl.ds(owner(i) * share2, mains[p])], main(y2_in, i, p),
            send_y.at[i, p], recv_y.at[i, p], y_peer,
        )

    def z_copy(i, p):
        at = 3 * inner if i == 0 else i
        return remote(
            main(z_out, i, p), main(z_in, at, p), send_z.at[i, p], recv_z.at[at, p],
            {"col": receiver(i)},
        )

    def z_arrival(at, p):
        remote(
            main(z_in, at, p), main(z_in, at, p), send_z.at[0, p], recv_z.at[at, p],
            {"col": receiver(0)},
        ).wait_recv()

    def near_sum(i, p, b):
        return home[p, owner(i) * share2 + b] + y2_in[i, p, b].astype(F32)

    def along_z(i, p):
        y_copy(i, p).wait_recv()

        def plain(b):
            z_out[i, p, b] = near_sum(i, p, b).astype(BF16)

        def joined(b):
            z_out[i, p, b] = (near_sum(i, p, b) + z_in[0, p, b].astype(F32)).astype(BF16)

        if i == 2:
            @pl.when(inner == 1)
            def _():
                z_arrival(0, p)
                each(mains[p], joined)

            @pl.when(inner == 0)
            def _():
                each(mains[p], plain)
        else:
            each(mains[p], plain)
        z_copy(i, p).start()

    def front_copy(i, h):
        at = 3 * inner if i == 0 else i
        return remote(
            front_out.at[i, h], front_in.at[at, h],
            send_f.at[i, h], recv_f.at[at, h], {"col": receiver(i)},
        )

    def front_arrival(at, h):
        remote(
            front_in.at[at, h], front_in.at[at, h],
            send_f.at[0, h], recv_f.at[at, h], {"col": receiver(0)},
        ).wait_recv()

    def front_send(i, h):
        def put(with_arrival):
            for b in range(fronts):
                value = front[h, owner(i) * fronts + b]
                if with_arrival:
                    value += front_in[0, h, b].astype(F32)
                front_out[i, h, b] = value.astype(BF16)

        if i == 2:
            @pl.when(inner == 1)
            def _():
                front_arrival(0, h)
                put(True)

            @pl.when(inner == 0)
            def _():
                put(False)
        else:
            put(False)
        front_copy(i, h).start()

    def front_total(h, slots):
        for at in slots:
            front_arrival(at, h)
        for b in range(fronts):
            value = front[h, c * fronts + b]
            for at in slots:
                value += front_in[at, h, b].astype(F32)
            if h:
                front_y_out[b] = value.astype(BF16)
            else:
                front[h, c * fronts + b] = value

    def by_place(work):
        @pl.when(inner == 1)
        def _():
            work((1, 2, 3))

        @pl.when(inner == 0)
        def _():
            work((1, 2))

    def front_close(h):
        by_place(functools.partial(front_total, h))
        if h:
            begin(remote(front_y_out, front_y_in, send_fy.at[0], recv_fy.at[0], y_peer))

    def put_out(p, b, value):
        value = jnp.maximum(value + bias2_v[b:b + 1, :], 0.0)
        out[p * size:(p + 1) * size, b * block:(b + 1) * block] = value.astype(BF16)

    def front_finish():
        arrived(front_y_in, send_fy.at[0], recv_fy.at[0])
        for b in range(fronts):
            put_out(0, mains[0] + b, front[0, c * fronts + b] + front_y_in[b].astype(F32))

    def finish(p, slots):
        for at in slots:
            z_arrival(at, p)
        for b in range(mains[p]):
            value = home[p, c * share2 + b] + y2_in[last, p, b].astype(F32)
            for at in slots:
                value += z_in[at, p, b].astype(F32)
            put_out(p, b, value)

    def finish_wait(p):
        y_copy(last, p).wait_recv()

    w1_load.wait()
    first_partial(0, 0)
    pass_on(0, 0)
    pair(0, 0)
    for part in range(1, parts):
        hand_over(1, part)
    for part in range(1, parts):
        pass_on(0, part)
    first_partial(0, 1)
    pass_on(1, 0)
    passed(0)
    first_partial(1, 0)
    pair(1, 0)
    along_y(1, 0)
    pair(0, 1)
    for part in range(1, parts):
        pass_on(1, part)
    arrived(live_in, live_sem.at[0], live_sem.at[1])
    along_x(1, 0)
    passed(1)
    first_partial(1, 1, lambda: along_y(0, 0))
    forward(1, 0)
    pair(1, 1)
    w2_load.wait()
    second_partial(1, 0, lambda: along_x(0, 0))
    for i in range(n_col):
        y_copy(i, 0).start()
    front_send(0, 1)
    front_send(1, 1)
    along_y(1, 1)
    along_y(0, 1)
    forward(0, 0)
    front_send(2, 1)
    second_partial(0, 0)
    along_x(1, 1)
    along_z(0, 0)
    front_send(0, 0)
    along_x(0, 1)
    along_z(1, 0)
    forward(1, 1)
    second_partial(1, 1)
    for i in range(n_col):
        y_copy(i, 1).start()
    along_z(2, 0)
    front_send(1, 0)
    front_close(1)
    forward(0, 1)
    second_partial(0, 1)
    front_send(2, 0)
    along_z(0, 1)
    finish_wait(0)
    by_place(functools.partial(finish, 0))
    along_z(1, 1)
    front_close(0)
    along_z(2, 1)
    finish_wait(1)
    front_finish()
    by_place(functools.partial(finish, 1))
    for copy in started:
        copy.wait_send()
    for i in range(n_col):
        for p in range(2):
            y_copy(i, p).wait_send()
            if i < last:
                z_copy(i, p).wait_send()
                front_copy(i, p).wait_send()


def fused_layers(acts, act_mask, w1, cols1, bias1, mask2, w2, cols2, bias2):
    block = w1.shape[-1]
    stored = w1.shape[0]
    rows = acts.shape[0]
    row_blocks, col_blocks = act_mask.shape[1], mask2.shape[1]
    n_row, n_col = lax.axis_size("row"), lax.axis_size("col")
    size = rows // 2
    share1 = col_blocks // 2 // n_row
    share2 = row_blocks // n_col
    fronts = share2 // 4
    flat1, flat2 = w1.reshape(-1, block, block), w2.reshape(-1, block, block)
    count = flat1.shape[0]
    half = col_blocks // 2
    parts = 4
    vmem = pl.BlockSpec(memory_space=pltpu.VMEM)
    hbm = pl.BlockSpec(memory_space=pltpu.HBM)
    tile = (size, block)
    dma = pltpu.SemaphoreType.DMA
    return pl.pallas_call(
        functools.partial(layers_kernel, n_col, fronts),
        out_shape=jax.ShapeDtypeStruct((rows, share2 * block), BF16),
        in_specs=[hbm] * 9,
        out_specs=vmem,
        scratch_shapes=[
            pltpu.VMEM((count, block, block), BF16),
            pltpu.VMEM((count, block, block), BF16),
            pltpu.VMEM((count + 1, *tile), F32),
            pltpu.VMEM((stored, *tile), BF16),
            pltpu.VMEM((stored, *tile), BF16),
            pltpu.VMEM((2, size, stored * block), BF16),
            pltpu.VMEM((2, size, stored // 2 * block), BF16),
            pltpu.VMEM((2, stored, *tile), BF16),
            pltpu.VMEM((2, stored // 2, *tile), BF16),
            pltpu.VMEM((row_blocks, rows), jnp.int32),
            pltpu.VMEM(cols1.shape[::-1], jnp.int32),
            pltpu.VMEM(cols2.shape[::-1], jnp.int32),
            pltpu.VMEM((col_blocks, rows), jnp.int32),
            pltpu.VMEM((col_blocks, block), F32),
            pltpu.VMEM((share2, block), F32),
            pltpu.VMEM((8, count), jnp.int32),
            pltpu.SMEM((8, count), jnp.int32),
            pltpu.VMEM((share1, rows), jnp.int32),
            pltpu.VMEM((2, 2, half, *tile), F32),
            pltpu.VMEM((2, 2, half, *tile), BF16),
            pltpu.VMEM((2, 2, half, *tile), BF16),
            pltpu.VMEM((2, 2, half // 2, *tile), BF16),
            pltpu.VMEM((2, 2, half // 2, *tile), BF16),
            pltpu.VMEM((2, 2, share1, *tile), BF16),
            pltpu.VMEM((2, 2, share1, *tile), BF16),
            pltpu.VMEM((half, *tile), BF16),
            pltpu.VMEM((half, *tile), BF16),
            pltpu.VMEM((half, *tile), BF16),
            pltpu.VMEM((half, *tile), BF16),
            pltpu.VMEM((2, row_blocks, *tile), BF16),
            pltpu.VMEM((2, row_blocks, *tile), F32),
            pltpu.VMEM((n_col, 2, share2, *tile), BF16),
            pltpu.VMEM((n_col - 1, 2, share2, *tile), BF16),
            pltpu.VMEM((n_col, 2, share2, *tile), BF16),
            pltpu.VMEM((2, n_col * fronts, *tile), F32),
            pltpu.VMEM((n_col - 1, 2, fronts, *tile), BF16),
            pltpu.VMEM((n_col, 2, fronts, *tile), BF16),
            pltpu.VMEM((fronts, *tile), BF16),
            pltpu.VMEM((fronts, *tile), BF16),
            dma((16,)),
            dma((2, 2, parts)),
            dma((2, 2, parts)),
            dma((2,)),
            dma((6, 2, 2)),
            dma((6, 2, 2)),
            dma((n_col, 2)),
            dma((n_col, 2)),
            dma((n_col - 1, 2)),
            dma((n_col, 2)),
            dma((n_col - 1, 2)),
            dma((n_col, 2)),
            dma((1,)),
            dma((1,)),
        ],
        compiler_params=pltpu.CompilerParams(
            collective_id=1, has_side_effects=True, vmem_limit_bytes=62 * 1024 * 1024
        ),
        name="layers",
    )(
        acts, act_mask.T, cols1.T, cols2.T, mask2.T, bias1.reshape(col_blocks, block),
        bias2.reshape(share2, block), flat1, flat2,
    )


def solution(mesh):
    near = mesh.shape["depth"] == 2 and mesh.shape["row"] == 4 and mesh.shape["col"] == 4
    return jax.shard_map(
        fused_layers if near else gathered_weights,
        mesh=mesh,
        in_specs=(
            P("depth", "row"),
            P("depth", "row"),
            P(("row", "depth"), "col", None, None),
            P("row", "col"),
            P("col"),
            P("depth", "col"),
            P(("col", "depth"), "row", None, None),
            P("col", "row"),
            P(("row", "col")),
        ),
        out_specs=P("depth", ("row", "col")),
        check_vma=False,
    )
```

```python
import functools

import jax
import jax.numpy as jnp
from jax import lax
from jax.experimental import pallas as pl
from jax.experimental.pallas import tpu as pltpu
from jax.sharding import PartitionSpec as P


def fold_function(inputs, targets, stride):

    def add_tiles(running_total, tiles, first_row):

        def advance(number, total):
            offset = number * stride
            block_list = lax.dynamic_slice_in_dim(tiles, offset, stride, 0)
            incoming_rows = lax.dynamic_slice_in_dim(inputs, offset, stride, 1)
            wanted = lax.dynamic_slice_in_dim(targets, offset, stride, 0)
            product = jnp.einsum(
                "tws,wish->twih", incoming_rows, block_list, preferred_element_type=jnp.float32
            )
            flat_product = product.reshape(product.shape[0], -1, product.shape[-1])
            return total.at[:, wanted.reshape(-1)].add(flat_product)

        return lax.fori_loop(0, tiles.shape[0] // stride, advance, running_total)

    return add_tiles


def gathered_weights(acts, act_mask, w1, cols1, bias1, mask2, w2, cols2, bias2):
    block = w1.shape[-1]
    rows_dev = acts.shape[0]
    row_blocks = act_mask.shape[1]
    col_blocks = mask2.shape[1]
    row_index = lax.axis_index("row")
    col_index = lax.axis_index("col")
    masked = acts.reshape(rows_dev, row_blocks, block) * act_mask[:, :, None].astype(jnp.bfloat16)
    first_layer_destinations = cols1 - col_index * col_blocks
    second_targets = cols2 - row_index * row_blocks
    first_offset_value = jnp.zeros((rows_dev, col_blocks, block), jnp.float32)
    first_fold = fold_function(masked, first_layer_destinations, w1.shape[0])
    first_sum = first_fold(
        first_offset_value, lax.all_gather(w1, "depth", axis=0, tiled=True), jnp.int32(0)
    )
    bias_blocks = bias1.reshape(col_blocks, block)
    share = col_blocks // lax.axis_size("row")
    part_sum = lax.psum_scatter(first_sum, "row", scatter_dimension=1, tiled=True)
    bias_part = lax.dynamic_slice_in_dim(bias_blocks, row_index * share, share, 0)
    mask_part = lax.dynamic_slice_in_dim(mask2, row_index * share, share, 1)
    hidden_part = jnp.maximum(part_sum + bias_part, 0.0) * mask_part[:, :, None].astype(jnp.float32)
    hidden = lax.all_gather(hidden_part.astype(jnp.bfloat16), "row", axis=1, tiled=True)
    second_start = jnp.zeros((rows_dev, row_blocks, block), jnp.float32)
    second_fold = fold_function(hidden, second_targets, w2.shape[0])
    second_sum = second_fold(
        second_start, lax.all_gather(w2, "depth", axis=0, tiled=True), jnp.int32(0)
    )
    outcome = lax.psum_scatter(second_sum, "col", scatter_dimension=1, tiled=True)
    bias_out = bias2.reshape(outcome.shape[1], block)
    return jnp.maximum(outcome + bias_out, 0.0).astype(jnp.bfloat16).reshape(rows_dev, -1)


MESH = pl.DeviceIdType.MESH
F32, BF16 = jnp.float32, jnp.bfloat16


def plan_rows(cols, first, stored):
    entries = cols.shape[0]
    count = stored * entries
    small = cols.astype(BF16)

    def iota(shape, dim):
        return lax.broadcasted_iota(jnp.int32, shape, dim).astype(F32)

    def row_of(j):
        return jnp.floor((j + 0.5) * (1.0 / entries))

    tall_shape = (cols.shape[1], count)
    spread = row_of(iota(tall_shape, 1)) + first.astype(F32) == iota(tall_shape, 0)
    spread = jnp.where(spread, 1.0, 0.0).astype(BF16)
    wide = jnp.dot(small, spread, preferred_element_type=F32)
    lane = iota((entries, count), 1)
    at = lane - row_of(lane) * entries == iota((entries, count), 0)
    col_row = jnp.sum(jnp.where(at, wide, 0.0), axis=0, keepdims=True)
    down_shape = (count, cols.shape[1])
    down = row_of(iota(down_shape, 0)) + first.astype(F32) == iota(down_shape, 1)
    down = jnp.where(down, 1.0, 0.0).astype(BF16)
    tall = lax.dot_general(down, small, (((1,), (1,)), ((), ())), preferred_element_type=F32)
    line = iota((count, entries), 0)
    at = line - row_of(line) * entries == iota((count, entries), 1)
    col_col = jnp.sum(jnp.where(at, tall, 0.0), axis=1, keepdims=True)
    index_row, index_col = iota((1, count), 1), iota((count, 1), 0)
    key_row, key_col = col_row * count + index_row, col_col * count + index_col

    def total(flags, axis):
        return jnp.sum(jnp.where(flags, 1.0, 0.0), axis=axis, keepdims=True)

    rank = total(key_row < key_col, 1)
    less = total(col_row < col_col, 1)
    hit = rank == iota((count, count), 1)
    entry = jnp.sum(jnp.where(hit, index_col, 0.0), axis=0, keepdims=True)
    same = jnp.sum(jnp.where(hit, jnp.where(rank > less, 1.0, 0.0), 0.0), axis=0, keepdims=True)
    upto, below = total(col_col <= index_row, 0), total(col_col < index_row, 0)
    last = jnp.where(upto > below, upto - 1.0, float(count))
    return [row_of(entry), entry, same, last]


def each(count, body, width=2):
    def step(at, carry):
        for u in range(width):
            body(at * width + u)
        return carry

    lax.fori_loop(0, count // width, step, 0)


def layers_kernel(
    n_col, fronts, acts, act_mask, cols1, cols2, mask2, bias1, bias2, w1, w2, out,
    wbuf, wbuf2, sums, acts_in0, acts_in1, keep_raw, give_raw, keep, give,
    act_mask_v, cols1_v, cols2_v, mask2_v, bias1_v, bias2_v, plan_v, plan, live_in,
    kept, given, core_in, y_out, y_in, x_out, x_in, xf_out, xf_in,
    x1_00, x1_01, x1_10, x1_11, away, home, y2_in, z_out, z_in,
    front, front_out, front_in, front_y_out, front_y_in,
    load_sem, acts_send, acts_recv, live_sem, send_sem, recv_sem,
    send_y, recv_y, send_z, recv_z, send_f, recv_f, send_fy, recv_fy, xf_send, xf_recv,
):
    r, c, d = lax.axis_index("row"), lax.axis_index("col"), lax.axis_index("depth")
    n_row = lax.axis_size("row")
    x, core = r // 2, r % 2
    partner = {"row": x * 2 + 1 - core}
    y_peer = {"depth": 1 - d}
    x_peer = {"row": (1 - x) * 2 + core}
    near = c % 2
    z_mate = {"col": c + 1 - 2 * near}
    entries, block = wbuf.shape[0], wbuf.shape[-1]
    size = sums.shape[1]
    stored = acts_in0.shape[0]
    share1 = x_in.shape[2]
    share2 = bias2.shape[0]
    acts_in = (acts_in0, acts_in1)
    x1 = ((x1_00, x1_01), (x1_10, x1_11))
    started = []

    loads = []

    def load(source, target):
        copy = pltpu.make_async_copy(source, target, load_sem.at[len(loads)])
        copy.start()
        loads.append(copy)
        return copy

    half_blocks = stored // 2
    give_first = pl.multiple_of((1 - d) * stored + near * half_blocks, half_blocks)
    keep_first = pl.multiple_of(d * stored, stored)
    mask_loads = [load(act_mask, act_mask_v)]
    give_loads = [
        load(
            acts.at[pl.ds(rc * size, size), pl.ds(give_first * block, half_blocks * block)],
            give_raw.at[rc],
        )
        for rc in range(2)
    ]
    plan_loads = [load(cols1, cols1_v), load(cols2, cols2_v)]
    keep_loads = [
        load(
            acts.at[pl.ds(rc * size, size), pl.ds(keep_first * block, stored * block)],
            keep_raw.at[rc],
        )
        for rc in range(2)
    ]
    small_loads = [load(mask2, mask2_v), load(bias1, bias1_v), load(bias2, bias2_v)]
    w1_load = load(w1, wbuf)
    w2_load = load(w2, wbuf2)

    barrier = pltpu.get_barrier_semaphore()
    greeted = [partner, y_peer, x_peer]
    greeted += [{"col": lax.rem(c + o, n_col)} for o in range(1, n_col)]
    for device in greeted:
        pl.semaphore_signal(barrier, inc=1, device_id=device, device_id_type=MESH)

    def remote(source, target, send, recv, device):
        return pltpu.make_async_remote_copy(
            src_ref=source, dst_ref=target, send_sem=send, recv_sem=recv,
            device_id=device, device_id_type=MESH,
        )

    def begin(copy):
        copy.start()
        started.append(copy)

    parts = acts_send.shape[2]
    piece_blocks = half_blocks // parts

    def piece(which, part):
        return pl.ds(which * half_blocks + part * piece_blocks, piece_blocks)

    def mask_blocks(first, count):
        rows = act_mask_v[pl.ds(first, count), :]
        return rows.astype(F32).T.astype(BF16)

    def hand_over(rc, part):
        begin(remote(
            give.at[rc, pl.ds(part * piece_blocks, piece_blocks)],
            acts_in[rc].at[piece(near, part)],
            acts_send.at[0, rc, part], acts_recv.at[0, rc, part], y_peer,
        ))

    for copy in mask_loads:
        copy.wait()
    give_mask = mask_blocks(give_first, half_blocks)
    for rc in range(2):
        give_loads[rc].wait()
        for b in range(half_blocks):
            give[rc, b] = (
                give_raw[rc, :, b * block:(b + 1) * block]
                * give_mask[rc * size:(rc + 1) * size, b:b + 1]
            )
        if rc == 0:
            pl.semaphore_wait(barrier, len(greeted))
        for part in range(1 if rc else parts):
            hand_over(rc, part)
    for copy in plan_loads:
        copy.wait()
    held = cols1.shape[1] // 2
    local1 = plan_rows((cols1_v[...] - c * n_row * 2 * share1).astype(F32), d * held, held)
    local2 = plan_rows((cols2_v[...] - r * n_col * share2).astype(F32), d * held, held)
    for n, value in enumerate(local1 + local2):
        top = (stored - 1, entries - 1, 1, entries)[n % 4]
        plan_v[n:n + 1, :] = jnp.clip(value.astype(jnp.int32), 0, top)
    plan_copy = load(plan_v, plan)
    keep_mask = mask_blocks(keep_first, stored)
    for rc in range(2):
        keep_loads[rc].wait()
        for b in range(stored):
            keep[rc, b] = (
                keep_raw[rc, :, b * block:(b + 1) * block]
                * keep_mask[rc * size:(rc + 1) * size, b:b + 1]
            )
    for copy in small_loads:
        copy.wait()
    share_rows = n_row * share1

    def live_rows(side):
        return mask2_v.at[pl.ds(pl.multiple_of(side * share_rows + r * share1, share1), share1)]

    begin(remote(live_rows(1 - d), live_in, live_sem.at[0], live_sem.at[1], y_peer))
    plan_copy.wait()

    def arrived(target, send, recv):
        remote(target, target, send, recv, y_peer).wait_recv()

    def pass_on(rc, part):
        mine = acts_in[rc].at[piece(near, part)]
        arrived(mine, acts_send.at[0, rc, part], acts_recv.at[0, rc, part])
        begin(remote(mine, mine, acts_send.at[1, rc, part], acts_recv.at[1, rc, part], z_mate))

    def passed(rc):
        for part in range(parts):
            theirs = acts_in[rc].at[piece(1 - near, part)]
            arrived(theirs, acts_send.at[1, rc, part], acts_recv.at[1, rc, part])

    sums[entries] = jnp.zeros(sums.shape[1:], F32)

    def multiply(x_ref, layer, between):
        weights = wbuf2 if layer else wbuf
        width = 128 if entries % 128 == 0 else 1

        def step(at, running):
            for u in range(width):
                p = at * width + u
                product = jnp.dot(
                    x_ref[plan[layer * 4, p]], weights[plan[layer * 4 + 1, p]],
                    preferred_element_type=F32,
                )
                running = running * plan[layer * 4 + 2, p].astype(F32) + product
                sums[p] = running
            return running

        steps = entries // width
        half_way = steps // 2 if between is not None else 0
        running = jnp.zeros(sums.shape[1:], F32)
        if between is not None:
            running = lax.fori_loop(0, half_way, step, running)
            between()
        lax.fori_loop(half_way, steps, step, running)

    def column(layer, b):
        return sums[plan[layer * 4 + 3, b]]

    def first_partial(h, rc, between=None):
        multiply(acts_in[rc] if h else keep.at[rc], 0, between)

        def split(q):
            at = (q // share1) * 2 * share1 + q % share1
            kept[h, rc, q] = column(0, at + core * share1)
            given[h, rc, q] = column(0, at + (1 - core) * share1).astype(BF16)

        each(kept.shape[2], split)
        send(0, given.at[h, rc], core_in.at[h, rc], h, rc, h, partner)

    def send(stage, source, target, h, rc, landing, device):
        begin(remote(
            source, target, send_sem.at[stage, h, rc], recv_sem.at[stage, landing, rc], device
        ))

    def await_stage(stage, target, h, rc):
        arrived(target, send_sem.at[stage, h, rc], recv_sem.at[stage, h, rc])

    half = kept.shape[2] // 2
    quarter = half // 2

    def pair(h, rc):
        await_stage(0, core_in.at[h, rc], h, rc)

        def other(q):
            at = (1 - d) * half + q
            y_out[h, rc, q] = (kept[h, rc, at] + core_in[h, rc, at].astype(F32)).astype(BF16)

        def own(q):
            at = d * half + q
            kept[h, rc, at] = kept[h, rc, at] + core_in[h, rc, at].astype(F32)

        each(half, other)
        send(1, y_out.at[h, rc], y_in.at[1 - h, rc], h, rc, 1 - h, y_peer)
        each(half, own)

    def pair_x():
        await_stage(0, core_in.at[0, 1], 0, 1)
        for side in (1 - d, d):
            def theirs(q):
                at = side * half + (1 - x) * quarter + q
                xf_out[side, q] = (kept[0, 1, at] + core_in[0, 1, at].astype(F32)).astype(BF16)

            each(quarter, theirs)
        side_send(1 - d, 0)
        for side in (1 - d, d):
            def mine(q):
                at = side * half + x * quarter + q
                kept[0, 1, at] = kept[0, 1, at] + core_in[0, 1, at].astype(F32)

            each(quarter, mine)

    def side_send(side, n):
        begin(remote(xf_out.at[side], xf_in.at[side], xf_send.at[n], xf_recv.at[n], x_peer))

    def other_part(row):
        return y_in.at[1, 1, pl.ds(row * quarter, quarter)]

    def settle_other():
        arrived(xf_in.at[1 - d], xf_send.at[0], xf_recv.at[0])

        def body(q):
            y_out[0, 1, q] = (
                kept[0, 1, (1 - d) * half + x * quarter + q] + xf_in[1 - d, q].astype(F32)
            ).astype(BF16)

        each(quarter, body)
        send(1, y_out.at[0, 1, pl.ds(0, quarter)], other_part(x), 0, 1, 1, y_peer)

    def settle_own():
        arrived(xf_in.at[d], xf_send.at[1], xf_recv.at[1])

        def body(q):
            at = d * half + x * quarter + q
            kept[0, 1, at] = kept[0, 1, at] + xf_in[d, q].astype(F32)

        each(quarter, body)

    def cross_1():
        def body(q):
            x_out[1, 1, q] = kept[1, 1, d * half + (1 - x) * quarter + q].astype(BF16)

        each(quarter, body)
        send(2, x_out.at[1, 1], x_in.at[1, 1], 1, 1, 1, x_peer)

    def cross_0():
        await_stage(1, y_in.at[0, 1], 0, 1)
        theirs = y_in.at[0, 1, pl.ds((1 - x) * quarter, quarter)]
        send(2, theirs, x_in.at[0, 1], 0, 1, 0, x_peer)

    def along_y(h, rc):
        await_stage(1, y_in.at[h, rc], h, rc)

        def body(q):
            at = (1 - x) * quarter + q
            x_out[h, rc, q] = (
                kept[h, rc, d * half + at] + y_in[h, rc, at].astype(F32)
            ).astype(BF16)

        each(quarter, body)
        send(2, x_out.at[h, rc], x_in.at[h, rc], h, rc, h, x_peer)

    def slot(h, rc, row):
        return x1[h][rc].at[pl.ds(row * share1, share1)]

    def along_x(h, rc):
        if (h, rc) == (1, 1):
            await_stage(1, other_part(x), 1, 1)
        await_stage(2, x_in.at[h, rc], h, rc)
        live = (live_in if h else live_rows(d))[...].astype(F32).T[rc * size:(rc + 1) * size]
        shift = bias1_v[pl.ds(pl.multiple_of((d * n_row + r) * share1, share1), share1), :]
        for b in range(share1):
            at = x * quarter + b
            z = (
                kept[h, rc, d * half + at] + y_in[h, rc, at].astype(F32)
                + x_in[h, rc, b].astype(F32)
            )
            value = jnp.maximum(z + shift[b:b + 1, :], 0.0) * live[:, b:b + 1]
            x1[h][rc][r * share1 + b] = value.astype(BF16)
        mine = slot(h, rc, r)
        send(3, mine, mine, h, rc, h, x_peer)
        send(4, mine, mine, h, rc, h, partner)

    def forward(h, rc):
        theirs = slot(h, rc, (1 - x) * 2 + core)
        await_stage(3, theirs, h, rc)
        send(5, theirs, theirs, h, rc, h, partner)

    def second_partial(h, rc, between=None):
        await_stage(4, slot(h, rc, x * 2 + 1 - core), h, rc)
        await_stage(5, slot(h, rc, (1 - x) * 2 + 1 - core), h, rc)
        multiply(x1[h][rc], 1, between)

        def body(b):
            if h:
                away[rc, b] = column(1, b).astype(BF16)
            else:
                home[rc, b] = column(1, b)

        each(home.shape[1], body)

        def ahead(q):
            front[h, q] = column(1, (q // fronts) * share2 + mains[0] + q % fronts)

        if rc == 0:
            each(n_col * fronts, ahead)

    mains = (share2 - fronts, share2)

    def main(ref, i, p):
        return ref.at[i, p, pl.ds(0, mains[p])]

    last = n_col - 1
    upper = c // 2
    inner = c + upper * (last - 2 * c)

    def mirrored(value):
        return value + upper * (last - 2 * value)

    def owner(i):
        end, mid = (3, 2, 1, 0)[i], (2, 0, 3, 1)[i]
        return mirrored(end + inner * (mid - end))

    def receiver(i):
        end, mid = (1, 2, 1)[i], (2, 0, 3)[i]
        return mirrored(end + inner * (mid - end))

    def y_copy(i, p):
        return remote(
            away.at[p, pl.ds(owner(i) * share2, mains[p])], main(y2_in, i, p),
            send_y.at[i, p], recv_y.at[i, p], y_peer,
        )

    def z_copy(i, p):
        at = 3 * inner if i == 0 else i
        return remote(
            main(z_out, i, p), main(z_in, at, p), send_z.at[i, p], recv_z.at[at, p],
            {"col": receiver(i)},
        )

    def z_arrival(at, p):
        remote(
            main(z_in, at, p), main(z_in, at, p), send_z.at[0, p], recv_z.at[at, p],
            {"col": receiver(0)},
        ).wait_recv()

    def near_sum(i, p, b):
        return home[p, owner(i) * share2 + b] + y2_in[i, p, b].astype(F32)

    def along_z(i, p):
        y_copy(i, p).wait_recv()

        def plain(b):
            z_out[i, p, b] = near_sum(i, p, b).astype(BF16)

        def joined(b):
            z_out[i, p, b] = (near_sum(i, p, b) + z_in[0, p, b].astype(F32)).astype(BF16)

        if i == 2:
            @pl.when(inner == 1)
            def _():
                z_arrival(0, p)
                each(mains[p], joined)

            @pl.when(inner == 0)
            def _():
                each(mains[p], plain)
        else:
            each(mains[p], plain)
        z_copy(i, p).start()

    def front_copy(i, h):
        at = 3 * inner if i == 0 else i
        return remote(
            front_out.at[i, h], front_in.at[at, h],
            send_f.at[i, h], recv_f.at[at, h], {"col": receiver(i)},
        )

    def front_arrival(at, h):
        remote(
            front_in.at[at, h], front_in.at[at, h],
            send_f.at[0, h], recv_f.at[at, h], {"col": receiver(0)},
        ).wait_recv()

    def front_send(i, h):
        def put(with_arrival):
            for b in range(fronts):
                value = front[h, owner(i) * fronts + b]
                if with_arrival:
                    value += front_in[0, h, b].astype(F32)
                front_out[i, h, b] = value.astype(BF16)

        if i == 2:
            @pl.when(inner == 1)
            def _():
                front_arrival(0, h)
                put(True)

            @pl.when(inner == 0)
            def _():
                put(False)
        else:
            put(False)
        front_copy(i, h).start()

    def front_total(h, slots):
        for at in slots:
            front_arrival(at, h)
        for b in range(fronts):
            value = front[h, c * fronts + b]
            for at in slots:
                value += front_in[at, h, b].astype(F32)
            if h:
                front_y_out[b] = value.astype(BF16)
            else:
                front[h, c * fronts + b] = value

    def by_place(work):
        @pl.when(inner == 1)
        def _():
            work((1, 2, 3))

        @pl.when(inner == 0)
        def _():
            work((1, 2))

    def front_close(h):
        by_place(functools.partial(front_total, h))
        if h:
            begin(remote(front_y_out, front_y_in, send_fy.at[0], recv_fy.at[0], y_peer))

    def put_out(p, b, value):
        value = jnp.maximum(value + bias2_v[b:b + 1, :], 0.0)
        out[p * size:(p + 1) * size, b * block:(b + 1) * block] = value.astype(BF16)

    def front_finish():
        arrived(front_y_in, send_fy.at[0], recv_fy.at[0])
        for b in range(fronts):
            put_out(0, mains[0] + b, front[0, c * fronts + b] + front_y_in[b].astype(F32))

    def finish(p, slots):
        for at in slots:
            z_arrival(at, p)
        for b in range(mains[p]):
            value = home[p, c * share2 + b] + y2_in[last, p, b].astype(F32)
            for at in slots:
                value += z_in[at, p, b].astype(F32)
            put_out(p, b, value)

    def finish_wait(p):
        y_copy(last, p).wait_recv()

    w1_load.wait()
    first_partial(0, 0)
    pass_on(0, 0)
    pair(0, 0)
    for part in range(1, parts):
        hand_over(1, part)
    for part in range(1, parts):
        pass_on(0, part)
    first_partial(0, 1)
    pass_on(1, 0)
    passed(0)
    first_partial(1, 0, pair_x)
    pair(1, 0)
    along_y(1, 0)
    side_send(d, 1)
    for part in range(1, parts):
        pass_on(1, part)
    settle_other()
    arrived(live_in, live_sem.at[0], live_sem.at[1])
    along_x(1, 0)
    passed(1)
    first_partial(1, 1, lambda: along_y(0, 0))
    forward(1, 0)
    pair(1, 1)
    cross_1()
    w2_load.wait()
    second_partial(1, 0, lambda: along_x(0, 0))
    for i in range(n_col):
        y_copy(i, 0).start()
    front_send(0, 1)
    front_send(1, 1)
    settle_own()
    along_x(1, 1)
    cross_0()
    forward(0, 0)
    front_send(2, 1)
    second_partial(0, 0)
    along_z(0, 0)
    front_send(0, 0)
    along_x(0, 1)
    along_z(1, 0)
    front_send(1, 0)
    forward(1, 1)
    second_partial(1, 1)
    for i in range(n_col):
        y_copy(i, 1).start()
    along_z(2, 0)
    front_close(1)
    forward(0, 1)
    second_partial(0, 1)
    front_send(2, 0)
    along_z(0, 1)
    finish_wait(0)
    by_place(functools.partial(finish, 0))
    along_z(1, 1)
    front_close(0)
    along_z(2, 1)
    finish_wait(1)
    front_finish()
    by_place(functools.partial(finish, 1))
    for copy in started:
        copy.wait_send()
    for i in range(n_col):
        for p in range(2):
            y_copy(i, p).wait_send()
            if i < last:
                z_copy(i, p).wait_send()
                front_copy(i, p).wait_send()


def fused_layers(acts, act_mask, w1, cols1, bias1, mask2, w2, cols2, bias2):
    block = w1.shape[-1]
    stored = w1.shape[0]
    rows = acts.shape[0]
    row_blocks, col_blocks = act_mask.shape[1], mask2.shape[1]
    n_row, n_col = lax.axis_size("row"), lax.axis_size("col")
    size = rows // 2
    share1 = col_blocks // 2 // n_row
    share2 = row_blocks // n_col
    fronts = share2 * 8 // 16
    flat1, flat2 = w1.reshape(-1, block, block), w2.reshape(-1, block, block)
    count = flat1.shape[0]
    half = col_blocks // 2
    parts = 4
    vmem = pl.BlockSpec(memory_space=pltpu.VMEM)
    hbm = pl.BlockSpec(memory_space=pltpu.HBM)
    tile = (size, block)
    dma = pltpu.SemaphoreType.DMA
    return pl.pallas_call(
        functools.partial(layers_kernel, n_col, fronts),
        out_shape=jax.ShapeDtypeStruct((rows, share2 * block), BF16),
        in_specs=[hbm] * 9,
        out_specs=vmem,
        scratch_shapes=[
            pltpu.VMEM((count, block, block), BF16),
            pltpu.VMEM((count, block, block), BF16),
            pltpu.VMEM((count + 1, *tile), F32),
            pltpu.VMEM((stored, *tile), BF16),
            pltpu.VMEM((stored, *tile), BF16),
            pltpu.VMEM((2, size, stored * block), BF16),
            pltpu.VMEM((2, size, stored // 2 * block), BF16),
            pltpu.VMEM((2, stored, *tile), BF16),
            pltpu.VMEM((2, stored // 2, *tile), BF16),
            pltpu.VMEM((row_blocks, rows), jnp.int32),
            pltpu.VMEM(cols1.shape[::-1], jnp.int32),
            pltpu.VMEM(cols2.shape[::-1], jnp.int32),
            pltpu.VMEM((col_blocks, rows), jnp.int32),
            pltpu.VMEM((col_blocks, block), F32),
            pltpu.VMEM((share2, block), F32),
            pltpu.VMEM((8, count), jnp.int32),
            pltpu.SMEM((8, count), jnp.int32),
            pltpu.VMEM((share1, rows), jnp.int32),
            pltpu.VMEM((2, 2, half, *tile), F32),
            pltpu.VMEM((2, 2, half, *tile), BF16),
            pltpu.VMEM((2, 2, half, *tile), BF16),
            pltpu.VMEM((2, 2, half // 2, *tile), BF16),
            pltpu.VMEM((2, 2, half // 2, *tile), BF16),
            pltpu.VMEM((2, 2, share1, *tile), BF16),
            pltpu.VMEM((2, 2, share1, *tile), BF16),
            pltpu.VMEM((2, share1, *tile), BF16),
            pltpu.VMEM((2, share1, *tile), BF16),
            pltpu.VMEM((half, *tile), BF16),
            pltpu.VMEM((half, *tile), BF16),
            pltpu.VMEM((half, *tile), BF16),
            pltpu.VMEM((half, *tile), BF16),
            pltpu.VMEM((2, row_blocks, *tile), BF16),
            pltpu.VMEM((2, row_blocks, *tile), F32),
            pltpu.VMEM((n_col, 2, share2, *tile), BF16),
            pltpu.VMEM((n_col - 1, 2, share2, *tile), BF16),
            pltpu.VMEM((n_col, 2, share2, *tile), BF16),
            pltpu.VMEM((2, n_col * fronts, *tile), F32),
            pltpu.VMEM((n_col - 1, 2, fronts, *tile), BF16),
            pltpu.VMEM((n_col, 2, fronts, *tile), BF16),
            pltpu.VMEM((fronts, *tile), BF16),
            pltpu.VMEM((fronts, *tile), BF16),
            dma((16,)),
            dma((2, 2, parts)),
            dma((2, 2, parts)),
            dma((2,)),
            dma((6, 2, 2)),
            dma((6, 2, 2)),
            dma((n_col, 2)),
            dma((n_col, 2)),
            dma((n_col - 1, 2)),
            dma((n_col, 2)),
            dma((n_col - 1, 2)),
            dma((n_col, 2)),
            dma((1,)),
            dma((1,)),
            dma((2,)),
            dma((2,)),
        ],
        compiler_params=pltpu.CompilerParams(
            collective_id=1, has_side_effects=True, vmem_limit_bytes=62 * 1024 * 1024
        ),
        name="layers",
    )(
        acts, act_mask.T, cols1.T, cols2.T, mask2.T, bias1.reshape(col_blocks, block),
        bias2.reshape(share2, block), flat1, flat2,
    )


def solution(mesh):
    near = mesh.shape["depth"] == 2 and mesh.shape["row"] == 4 and mesh.shape["col"] == 4
    return jax.shard_map(
        fused_layers if near else gathered_weights,
        mesh=mesh,
        in_specs=(
            P("depth", "row"),
            P("depth", "row"),
            P(("row", "depth"), "col", None, None),
            P("row", "col"),
            P("col"),
            P("depth", "col"),
            P(("col", "depth"), "row", None, None),
            P("col", "row"),
            P(("row", "col")),
        ),
        out_specs=P("depth", ("row", "col")),
        check_vma=False,
    )
```
